256 devices in a mesh: section: 4 (over x), depth: 64 (over z, y, core).
Axes of the slice: x: 4, y: 4, z: 8, core: 2. Of those that a mesh axis runs over, the one named last changes fastest.
Arguments:
- activations: float32 [4, 4, 128, 64, 256], P('section', None, 'depth'), may hold values from -6 to 6
- filters: float32 [4, 27, 64, 64], P('section'), may hold values from -0.15625 to 0.15625
- cotangent: float32 [4, 128, 64, 256], P(None, 'depth'), may hold values from -6 to 6
Outputs:
- input_grads: float32 [4, 4, 128, 64, 256], P('section', None, 'depth')
- filter_grads: float32 [4, 27, 64, 64], P('section')
The draws below stay inside these ranges and needn't reach their ends.
All inputs are finite; a program needn't handle non-finite values.
Results may differ from the reference program's by a relative error of at most 0.0003.
Values sent between devices are 32-bit elements; how exact they have to be, the bound alone decides.
No kernel may reach another device: no remote copies, remote signals or barrier semaphores. Data moves between devices by JAX's collectives and lax.ppermute only.
A program may use at most 128 MiB of HBM per device.

```python
import math
import jax
import jax.numpy as jnp
from jax import lax

C = 64
H = 16
W = 16
MB = 4
SECTIONS = 4
DEPTH = 128
N_SECTION = 4


def level_of(rng, shape, split, least, largest):
    gain, own = 1.0, jax.random.fold_in(rng, 6)
    for dim, blocks in split:
        draws = jnp.exp(jax.random.uniform(jax.random.fold_in(own, dim), (blocks,), jnp.float32, least / len(split), largest / len(split)))
        gain = gain * jnp.repeat(draws, shape[dim] // blocks).reshape([-1 if axis == dim else 1 for axis in range(len(shape))])
    return gain


def gaussian(stream_key, dims, spread, bound, shards=(), dtype=jnp.bfloat16):
    loudness = level_of(stream_key, dims, shards, -0.22, 0.18) if shards else 1.0
    values = jax.random.normal(stream_key, dims, jnp.float32) * spread * loudness
    return jnp.minimum(jnp.maximum(values, -bound), bound).astype(dtype)


def setup_inputs(seed: int = 0) -> dict:
    streams_of = jax.random.split(jax.random.key(seed), 4)
    return {
        "activations": gaussian(streams_of[0], (SECTIONS, MB, DEPTH, C, H * W), 1.0, 6.0, ((0, 4), (2, 64)), jnp.float32),
        "filters": gaussian(streams_of[1], (SECTIONS, 27, C, C), (27 * C) ** -0.5, 0.15625, ((0, 4),), jnp.float32),
        "cotangent": gaussian(streams_of[2], (MB, DEPTH, C, H * W), 1.0, 6.0, ((1, 64),), jnp.float32),
    }


def convolve(volume, kernel_taps):
    depth_cells, channels, columns = volume.shape
    volume_grid = volume.reshape(1, depth_cells, channels, H, W).transpose(0, 2, 1, 3, 4)
    kernel = kernel_taps.reshape(3, 3, 3, channels, channels).transpose(3, 4, 0, 1, 2)
    result = lax.conv_general_dilated(volume_grid, kernel, (1, 1, 1), ((1, 1), (1, 1), (1, 1)), dimension_numbers=('NCDHW', 'OIDHW', 'NCDHW'), precision=lax.Precision.HIGHEST)
    return result[0].transpose(1, 0, 2, 3).reshape(depth_cells, channels, columns)

def silu_slope(preact):
    sigmoid_value = jax.nn.sigmoid(preact)
    return sigmoid_value * (1.0 + preact * (1.0 - sigmoid_value))

def reference(activations, filters, cotangent):
    upstream = [cotangent[micro_index] for micro_index in range(MB)]
    grad_layers = [None] * N_SECTION
    filter_layers = [None] * N_SECTION
    for layer_index in reversed(range(N_SECTION)):
        summed = jnp.zeros(filters.shape[1:], jnp.float32)
        outgoing = []
        for micro_index in range(MB):
            preact, pullback = jax.vjp(convolve, activations[layer_index, micro_index], filters[layer_index])
            slopes = upstream[micro_index] * silu_slope(preact)
            backward, filter_term = pullback(slopes)
            summed = summed + filter_term
            outgoing.append(backward)
        grad_layers[layer_index] = jnp.stack(outgoing)
        filter_layers[layer_index] = summed
        upstream = outgoing
    scaling = 1.0 / math.sqrt(MB * DEPTH * H * W)
    return (jnp.stack(grad_layers), jnp.stack(filter_layers) * scaling)
```

```python
import functools
import math

import jax
import jax.numpy as jnp
from jax import lax
from jax.experimental import pallas as pl
from jax.experimental.pallas import tpu as pltpu
from jax.sharding import Mesh
from jax.sharding import PartitionSpec as P

H = 16
W = 16
C = 64
DEPTH = ("depth_0", "depth_1", "depth_2")
PLANE = ("depth_0", "depth_1")
CORE = "depth_2"
N = 4
F32 = jnp.float32
BF16 = jnp.bfloat16
VMEM = pl.BlockSpec(memory_space=pltpu.VMEM)
SMEM = pl.BlockSpec(memory_space=pltpu.SMEM)


def run(body, args, outs, scratch=(), flops=0, name=None):
    nbytes = sum(a.size * a.dtype.itemsize for a in args)
    return pl.pallas_call(
        body,
        out_shape=[jax.ShapeDtypeStruct(s, t) for s, t in outs],
        in_specs=[SMEM] + [VMEM] * (len(args) - 1),
        out_specs=[VMEM] * len(outs),
        scratch_shapes=[pltpu.VMEM(s, t) for s, t in scratch],
        cost_estimate=pl.CostEstimate(flops=flops, bytes_accessed=nbytes, transcendentals=0),
        name=name,
    )(*args)


def split(x):
    high = x.astype(BF16)
    return high, (x - high.astype(F32)).astype(BF16)


def columns():
    return lax.broadcasted_iota(jnp.int32, (C, H * W), 1)


def across(x):
    place = columns()
    left = jnp.where(place % W == 0, 0.0, pltpu.roll(x, 1, 1))
    right = jnp.where(place % W == W - 1, 0.0, pltpu.roll(x, H * W - 1, 1))
    return jnp.concatenate([left, x, right], axis=0)


def down(x):
    return jnp.where(columns() < W, 0.0, pltpu.roll(x, W, 1))


def up(x):
    return jnp.where(columns() >= H * W - W, 0.0, pltpu.roll(x, H * W - W, 1))


def dot(a, b):
    return jnp.dot(a, b, preferred_element_type=F32)


def conv(taps, high, low):
    first = dot(taps, high)
    z = first[:192] + first[192:] + dot(taps[:192], low)
    return z[C : 2 * C] + down(z[:C]) + up(z[2 * C :])


def silu_slope(preact):
    gate = 1.0 / (1.0 + jnp.exp(-preact))
    return gate * (1.0 + preact * (1.0 - gate))


def forward_taps(filters):
    t = filters.reshape(3, 3, 3, C, C)
    return t.transpose(1, 3, 0, 2, 4).reshape(3 * C, 9 * C)


def backward_taps(filters):
    t = jnp.flip(filters, 0).reshape(3, 3, 3, C, C)
    return t.transpose(1, 4, 0, 2, 3).reshape(3 * C, 9 * C)


def slope_body(s_ref, act_ref, left_ref, right_ref, taps_ref, d0, d1, d2, d3, vh_ref, vl_ref, taps):
    s = s_ref[0]
    th, tl = split(taps_ref[...])
    taps[0:192] = th
    taps[192:384] = tl
    for k, out in enumerate((d0, d1, d2, d3)):
        m = (s + k) % N
        for e in range(4):
            if e == 0:
                x = left_ref[m]
            elif e == 3:
                x = right_ref[m]
            else:
                x = act_ref[m, e - 1]
            high, low = split(across(x))
            vh_ref[k, e] = high
            vl_ref[k, e] = low
        for d in range(2):
            z = conv(taps[...], vh_ref[k, d : d + 3].reshape(576, 256), vl_ref[k, d : d + 3].reshape(576, 256))
            out[d] = silu_slope(z)


def pick_body(s_ref, d0, d1, d2, d3, cot_ref, all_ref, s3_ref, to_right, to_left):
    m = s_ref[0]
    for k, ref in enumerate((d0, d1, d2, d3)):
        all_ref[(m + N - k) % N] = ref[...]
    top = cot_ref[m] * all_ref[3]
    s3_ref[...] = top
    to_right[0:2] = top
    to_right[2] = all_ref[2, 1]
    to_left[0:2] = top
    to_left[2] = all_ref[2, 0]


def taps_body(s_ref, own_ref, below_ref, above_ref, far0_ref, far1_ref, other_ref, out_ref):
    s = s_ref[0]
    c = s_ref[1]

    def put(layer, row, x):
        high, low = split(x)
        size = x.shape[0]
        out_ref[layer, pl.ds(row, size)] = high
        out_ref[layer, pl.ds(192 + row, size)] = low

    put(s, 0, own_ref[...])
    mine = pl.multiple_of(c * 96, 32)
    yours = pl.multiple_of((1 - c) * 96, 32)
    put((s + 3) % N, mine, below_ref[...])
    put((s + 1) % N, mine, above_ref[...])
    put((s + 2) % N, mine, jnp.concatenate([far0_ref[...], far1_ref[...]], axis=0))
    put((s + 3) % N, yours, other_ref[0:96])
    put((s + 1) % N, yours, other_ref[96:192])
    put((s + 2) % N, yours, other_ref[192:288])


def chain_body(layer, s_ref, left_ref, right_ref, all_ref, mid_ref, taps_ref, *refs):
    if layer == 3:
        ig_a, below_ref, ig_b, next_ref, to_right, to_left, vh, vl, wh, wl = refs
    else:
        ig_a, below_ref, ig_b, vh, vl, wh, wl = refs
    for e in range(6):
        x = left_ref[e] if e < 2 else (mid_ref[e - 2] if e < 4 else right_ref[e - 4])
        high, low = split(across(x))
        vh[e] = high
        vl[e] = low
    for d in range(4):
        g = conv(taps_ref[layer], vh[d : d + 3].reshape(576, 256), vl[d : d + 3].reshape(576, 256))
        factor = left_ref[2] if d == 0 else (right_ref[2] if d == 3 else all_ref[layer - 1, d - 1])
        slope = g * factor
        if 0 < d < 3:
            ig_a[d - 1] = g
            below_ref[d - 1] = slope
        high, low = split(across(slope))
        wh[d] = high
        wl[d] = low
    for d in range(2):
        g = conv(taps_ref[layer - 1], wh[d : d + 3].reshape(576, 256), wl[d : d + 3].reshape(576, 256))
        ig_b[d] = g
        if layer == 3:
            slope = g * all_ref[1, d]
            next_ref[d] = slope
            to_right[d] = slope
            to_left[d] = slope
    if layer == 3:
        to_right[2] = all_ref[0, 1]
        to_left[2] = all_ref[0, 0]


def pack_body(s_ref, x0, x1, x2, x3, o0, o1, o2, o3):
    m = s_ref[0]
    for layer, ref in enumerate((x0, x1, x2, x3)):
        k = (layer + N - m) % N
        for j, out in enumerate((o0, o1, o2, o3)):

            @pl.when(k == j)
            def _():
                out[...] = ref[...]


def filter_body(s_ref, g0, g1, g2, g3, vh_ref, vl_ref, keep_ref, send_ref, acc):
    c = s_ref[1]
    nt = (((1,), (1,)), ((), ()))
    for k, ref in enumerate((g0, g1, g2, g3)):
        for d in range(2):
            x = ref[d]
            high, low = split(jnp.concatenate([up(x), x, down(x)], axis=0))
            v = (N - k) % N
            right_high = vh_ref[v, d : d + 3].reshape(576, 256)
            right_low = vl_ref[v, d : d + 3].reshape(576, 256)
            first = lax.dot_general(jnp.concatenate([high, low], axis=0), right_high, nt, preferred_element_type=F32)
            z = first[:192] + first[192:] + lax.dot_general(high, right_low, nt, preferred_element_type=F32)
            if k == 0 and d == 0:
                acc[...] = z
            else:
                acc[...] += z

    def piece(row, size):
        if row < 768:
            j = row // 192
            return acc[row - j * 192 : row - j * 192 + size, j * 128 : (j + 1) * 128]
        r = row - 768
        return jnp.concatenate([acc[r : r + size, 512:576], acc[r + 96 : r + 96 + size, 512:576]], axis=1)

    for half in range(2):

        def fill(ref):
            row = 432 * half
            stop = row + 432
            while row < stop:
                size = min((row // 192 + 1) * 192 if row < 768 else 864, stop) - row
                ref[row - 432 * half : row - 432 * half + size] = piece(row, size)
                row += size
            ref[432:512] = jnp.zeros((80, 128), F32)

        @pl.when(c == half)
        def _():
            fill(keep_ref)

        @pl.when(c != half)
        def _():
            fill(send_ref)


def finish_body(s_ref, own_ref, other_ref, out_ref, full):
    c = s_ref[1]
    full[pl.ds(pl.multiple_of(c * 432, 8), 432)] = own_ref[0:432]
    full[pl.ds(pl.multiple_of((1 - c) * 432, 8), 432)] = other_ref[0:432]
    for a in range(3):
        for b in range(3):
            for cc in range(3):
                block = a * 3 + cc
                if block < 8:
                    x = full[(block // 2) * 192 + b * C : (block // 2) * 192 + b * C + C]
                    x = x[:, (block % 2) * C : (block % 2) * C + C]
                    out_ref[0, a * 9 + b * 3 + cc] = x
                else:
                    for part in range(2):
                        row = b * C + part * 32
                        side = 0 if row < 96 else 1
                        x = full[768 + row - 96 * side : 768 + row - 96 * side + 32, side * C : side * C + C]
                        out_ref[0, a * 9 + b * 3 + cc, part * 32 : part * 32 + 32] = x


def gather_body(s_ref, x0, x1, x2, x3, out_ref):
    s = s_ref[0]
    for k, ref in enumerate((x0, x1, x2, x3)):
        out_ref[0, (s + N - k) % N] = ref[...]


def shift(x, by):
    return lax.ppermute(x, "section", [(i, (i + by) % N) for i in range(N)])


def neighbours(to_right, to_left):
    count = lax.axis_size(DEPTH)
    return (
        lax.ppermute(to_right, DEPTH, [(i, i + 1) for i in range(count - 1)]),
        lax.ppermute(to_left, DEPTH, [(i + 1, i) for i in range(count - 1)]),
    )


def per_device(activations, filters, cotangent):
    s = lax.axis_index("section")
    c = lax.axis_index(CORE)
    place = jnp.stack([s, c]).astype(jnp.int32)
    act = activations[0]
    plane = (C, H * W)
    two = ((2, *plane), F32)
    three = ((3, *plane), F32)

    left, right = neighbours(act[:, 1], act[:, 0])

    own = backward_taps(filters[0])
    half = lax.dynamic_slice_in_dim(own, c * 96, 96, 0)
    below = shift(half, 1)
    above = shift(half, -1)
    far0 = shift(below[:48], 1)
    far1 = shift(above[48:], -1)
    mine = jnp.concatenate([below, above, far0, far1], axis=0)
    other = lax.ppermute(mine, CORE, [(0, 1), (1, 0)])

    *factors, vh, vl = run(
        slope_body,
        (place, act, left, right, forward_taps(filters[0])),
        [two] * 4 + [((N, 4, 192, 256), BF16)] * 2,
        [((384, 576), BF16)],
        flops=2 * 8 * 192 * 576 * 256 * 3,
        name="slope",
    )
    factors = [factors[0]] + [shift(factors[k], k) for k in (1, 2, 3)]

    (taps,) = run(
        taps_body, (place, own, below, above, far0, far1, other), [((N, 384, 576), BF16)], flops=10**6, name="taps"
    )

    every, s3, to_right, to_left = run(
        pick_body, (place, *factors, cotangent), [((N, 2, *plane), F32), two, three, three], flops=10**6, name="pick"
    )
    left, right = neighbours(to_right, to_left)
    scratch = [((6, 192, 256), BF16)] * 2 + [((4, 192, 256), BF16)] * 2
    ig3, s2, ig2, s1, to_right, to_left = run(
        functools.partial(chain_body, 3),
        (place, left, right, every, s3, taps),
        [two, two, two, two, three, three],
        scratch,
        flops=2 * 6 * 192 * 576 * 256 * 3,
        name="chain_top",
    )
    left, right = neighbours(to_right, to_left)
    ig1, s0, ig0 = run(
        functools.partial(chain_body, 1),
        (place, left, right, every, s1, taps),
        [two, two, two],
        scratch,
        flops=2 * 6 * 192 * 576 * 256 * 3,
        name="chain_low",
    )
    slopes = run(pack_body, (place, s0, s1, s2, s3), [two] * 4, flops=10**6, name="pack_slopes")
    slopes = [slopes[0]] + [shift(slopes[k], k) for k in (1, 2, 3)]
    grads = run(pack_body, (place, ig0, ig1, ig2, ig3), [two] * 4, flops=10**6, name="pack_grads")
    grads = [grads[0]] + [shift(grads[k], k) for k in (1, 2, 3)]

    keep, send = run(
        filter_body,
        (place, *slopes, vh, vl),
        [((512, 128), F32)] * 2,
        [((192, 576), F32)],
        flops=2 * 8 * 192 * 576 * 256 * 3,
        name="filter",
    )
    part = (keep + lax.ppermute(send, CORE, [(0, 1), (1, 0)])).reshape(32, 16, 128)
    part = lax.all_to_all(part, PLANE, 0, 0, tiled=True)
    scaling = 1.0 / math.sqrt(N * 2 * lax.axis_size(DEPTH) * H * W)
    total = jnp.sum(part, axis=0) * scaling
    part = lax.all_to_all(jnp.broadcast_to(total[None], (32, 16, 128)), PLANE, 0, 0, tiled=True).reshape(512, 128)
    other_part = lax.ppermute(part, CORE, [(0, 1), (1, 0)])
    (filter_grads,) = run(
        finish_body, (place, part, other_part), [((1, 27, C, C), F32)], [((864, 128), F32)], flops=10**6, name="finish"
    )
    (input_grads,) = run(gather_body, (place, *grads), [((1, N, 2, *plane), F32)], flops=10**6, name="gather")
    return input_grads, filter_grads


def solution(mesh):
    finer = Mesh(
        mesh.devices.reshape(mesh.shape["section"], 8, 4, 2),
        ("section", "depth_0", "depth_1", "depth_2"),
    )
    placed = (
        P("section", None, DEPTH, None, None),
        P("section", None, None, None),
        P(None, DEPTH, None, None),
    )
    return jax.shard_map(
        per_device,
        mesh=finer,
        in_specs=placed,
        out_specs=(P("section", None, DEPTH, None, None), P("section", None, None, None)),
        check_vma=False,
    )
```

```python
import math

import jax
import jax.numpy as jnp
from jax import lax
from jax.experimental import pallas as pl
from jax.experimental.pallas import tpu as pltpu
from jax.sharding import Mesh
from jax.sharding import PartitionSpec as P


H = 16
W = 16
C = 64
DEPTH = ("depth_0", "depth_1", "depth_2")
PLANE = ("depth_0", "depth_1")
CORE = "depth_2"
N = 4
F32 = jnp.float32
BF16 = jnp.bfloat16
LIMIT = 24 * 2**20
VMEM = pl.BlockSpec(memory_space=pltpu.VMEM)
SMEM = pl.BlockSpec(memory_space=pltpu.SMEM)


def run(body, args, outs, scratch=(), flops=0):
    nbytes = sum(a.size * a.dtype.itemsize for a in args)
    return pl.pallas_call(
        body,
        out_shape=[jax.ShapeDtypeStruct(s, t) for s, t in outs],
        in_specs=[SMEM] + [VMEM] * (len(args) - 1),
        out_specs=[VMEM] * len(outs),
        scratch_shapes=[pltpu.VMEM(s, t) for s, t in scratch],
        cost_estimate=pl.CostEstimate(flops=flops, bytes_accessed=nbytes, transcendentals=0),
        compiler_params=pltpu.CompilerParams(vmem_limit_bytes=LIMIT),
    )(*args)


def split(x):
    high = x.astype(BF16)
    return high, (x - high.astype(F32)).astype(BF16)


def columns():
    return lax.broadcasted_iota(jnp.int32, (C, H * W), 1)


def across(x):
    place = columns()
    left = jnp.where(place % W == 0, 0.0, pltpu.roll(x, 1, 1))
    right = jnp.where(place % W == W - 1, 0.0, pltpu.roll(x, H * W - 1, 1))
    return jnp.concatenate([left, x, right], axis=0)


def down(x):
    return jnp.where(columns() < W, 0.0, pltpu.roll(x, W, 1))


def up(x):
    return jnp.where(columns() >= H * W - W, 0.0, pltpu.roll(x, H * W - W, 1))


def dot(a, b):
    return jnp.dot(a, b, preferred_element_type=F32)


def conv(taps, high, low):
    first = dot(taps, high)
    z = first[:192] + first[192:] + dot(taps[:192], low)
    return z[C : 2 * C] + down(z[:C]) + up(z[2 * C :])


def silu_slope(preact):
    gate = 1.0 / (1.0 + jnp.exp(-preact))
    return gate * (1.0 + preact * (1.0 - gate))


def prepare_body(s_ref, f_ref, forward_ref, mine_ref, yours_ref, back):
    for b in range(3):
        rows = slice(b * C, b * C + C)
        low_rows = slice(192 + b * C, 192 + b * C + C)
        taps = [f_ref[0, a * 9 + b * 3 + cc] for a in range(3) for cc in range(3)]
        high, low = split(jnp.concatenate(taps, axis=1))
        forward_ref[rows] = high
        forward_ref[low_rows] = low
        taps = [f_ref[0, (2 - a) * 9 + (2 - b) * 3 + 2 - cc] for a in range(3) for cc in range(3)]
        back[rows] = jnp.concatenate(taps, axis=0).T
    c = s_ref[1]
    mine_ref[...] = back[pl.ds(pl.multiple_of(c * 96, 32), 96)]
    yours_ref[...] = back[pl.ds(pl.multiple_of((1 - c) * 96, 32), 96)]


def slope_body(s_ref, act_ref, left_ref, right_ref, taps_ref, d0, d1, d2, d3, vh_ref, vl_ref):
    s = s_ref[0]
    for k, out in enumerate((d0, d1, d2, d3)):
        m = (s + k) % N
        for e in range(4):
            if e == 0:
                x = left_ref[m]
            elif e == 3:
                x = right_ref[m]
            else:
                x = act_ref[m, e - 1]
            high, low = split(across(x))
            vh_ref[k, e] = high
            vl_ref[k, e] = low
        for d in range(2):
            z = conv(taps_ref[...], vh_ref[k, d : d + 3].reshape(576, 256), vl_ref[k, d : d + 3].reshape(576, 256))
            out[d] = silu_slope(z)


def chosen(index, refs, *at):
    out = refs[0][at]
    for k in range(1, len(refs)):
        out = jnp.where(index == k, refs[k][at], out)
    return out


def pick_body(s_ref, d0, d1, d2, d3, cot_ref, s3_ref, to_right, to_left):
    m = s_ref[0]
    refs = (d0, d1, d2, d3)
    for d in range(2):
        top = cot_ref[m, d] * chosen((m + N - 3) % N, refs, d)
        s3_ref[d] = top
        to_right[d] = top
        to_left[d] = top
    to_right[2] = chosen((m + N - 2) % N, refs, 1)
    to_left[2] = chosen((m + N - 2) % N, refs, 0)


def taps_body(s_ref, mine_ref, yours_ref, below_ref, above_ref, far0_ref, far1_ref, other_ref, out_ref):
    s = s_ref[0]
    c = s_ref[1]

    def put(layer, row, x):
        high, low = split(x)
        size = x.shape[0]
        out_ref[layer, pl.ds(row, size)] = high
        out_ref[layer, pl.ds(192 + row, size)] = low

    mine = pl.multiple_of(c * 96, 32)
    yours = pl.multiple_of((1 - c) * 96, 32)
    put(s, mine, mine_ref[...])
    put(s, yours, yours_ref[...])
    put((s + 3) % N, mine, below_ref[...])
    put((s + 1) % N, mine, above_ref[...])
    put((s + 2) % N, mine, jnp.concatenate([far0_ref[...], far1_ref[...]], axis=0))
    put((s + 3) % N, yours, other_ref[0:96])
    put((s + 1) % N, yours, other_ref[96:192])
    put((s + 2) % N, yours, other_ref[192:288])


def two_layers(layer, m, left_ref, right_ref, factors, mid_ref, taps_ref, ig_a, slope_a, vh, vl, wh, wl):
    for e in range(6):
        x = left_ref[e] if e < 2 else (mid_ref[e - 2] if e < 4 else right_ref[e - 4])
        high, low = split(across(x))
        vh[e] = high
        vl[e] = low
    for d in range(4):
        g = conv(taps_ref[layer], vh[d : d + 3].reshape(576, 256), vl[d : d + 3].reshape(576, 256))
        if d == 0:
            factor = left_ref[2]
        elif d == 3:
            factor = right_ref[2]
        else:
            factor = chosen((m + N - layer + 1) % N, factors, d - 1)
        slope = g * factor
        if 0 < d < 3:
            ig_a[d - 1] = g
            slope_a[d - 1] = slope
        high, low = split(across(slope))
        wh[d] = high
        wl[d] = low
    return [
        conv(taps_ref[layer - 1], wh[d : d + 3].reshape(576, 256), wl[d : d + 3].reshape(576, 256)) for d in range(2)
    ]


def top_body(s_ref, left_ref, right_ref, d0, d1, d2, d3, s3_ref, taps_ref, *refs):
    ig3, s2, ig2, s1, to_right, to_left, vh, vl, wh, wl = refs
    m = s_ref[0]
    factors = (d0, d1, d2, d3)
    grads = two_layers(3, m, left_ref, right_ref, factors, s3_ref, taps_ref, ig3, s2, vh, vl, wh, wl)
    for d, g in enumerate(grads):
        ig2[d] = g
        slope = g * chosen((m + N - 1) % N, factors, d)
        s1[d] = slope
        to_right[d] = slope
        to_left[d] = slope
    to_right[2] = chosen(m, factors, 1)
    to_left[2] = chosen(m, factors, 0)


def low_body(s_ref, left_ref, right_ref, d0, d1, d2, d3, s3, s2, s1, ig3, ig2, taps_ref, *refs):
    o, p, s0, ig1, ig0, vh, vl, wh, wl = refs[:4], refs[4:8], *refs[8:]
    m = s_ref[0]
    grads = two_layers(1, m, left_ref, right_ref, (d0, d1, d2, d3), s1, taps_ref, ig1, s0, vh, vl, wh, wl)
    for d in range(2):
        ig0[d] = grads[d]
        for k in range(N):
            o[k][d] = chosen((m + k) % N, (s0, s1, s2, s3), d)
            p[k][d] = chosen((m + k) % N, (ig0, ig1, ig2, ig3), d)


def filter_body(s_ref, g0, g1, g2, g3, vh_ref, vl_ref, keep_ref, send_ref, acc):
    c = s_ref[1]
    nt = (((1,), (1,)), ((), ()))
    for k, ref in enumerate((g0, g1, g2, g3)):
        for d in range(2):
            x = ref[d]
            high, low = split(jnp.concatenate([up(x), x, down(x)], axis=0))
            v = (N - k) % N
            right_high = vh_ref[v, d : d + 3].reshape(576, 256)
            right_low = vl_ref[v, d : d + 3].reshape(576, 256)
            first = lax.dot_general(jnp.concatenate([high, low], axis=0), right_high, nt, preferred_element_type=F32)
            z = first[:192] + first[192:] + lax.dot_general(high, right_low, nt, preferred_element_type=F32)
            if k == 0 and d == 0:
                acc[...] = z
            else:
                acc[...] += z

    def piece(row, size):
        if row < 768:
            j = row // 192
            return acc[row - j * 192 : row - j * 192 + size, j * 128 : (j + 1) * 128]
        r = row - 768
        return jnp.concatenate([acc[r : r + size, 512:576], acc[r + 96 : r + 96 + size, 512:576]], axis=1)

    for half in range(2):

        def fill(ref):
            row = 432 * half
            stop = row + 432
            while row < stop:
                size = min((row // 192 + 1) * 192 if row < 768 else 864, stop) - row
                ref[row - 432 * half : row - 432 * half + size] = piece(row, size)
                row += size
            ref[432:512] = jnp.zeros((80, 128), F32)

        @pl.when(c == half)
        def _():
            fill(keep_ref)

        @pl.when(c != half)
        def _():
            fill(send_ref)


def finish_body(s_ref, own_ref, other_ref, out_ref, full):
    c = s_ref[1]
    full[pl.ds(pl.multiple_of(c * 432, 8), 432)] = own_ref[0:432]
    full[pl.ds(pl.multiple_of((1 - c) * 432, 8), 432)] = other_ref[0:432]
    for a in range(3):
        for b in range(3):
            for cc in range(3):
                block = a * 3 + cc
                if block < 8:
                    x = full[(block // 2) * 192 + b * C : (block // 2) * 192 + b * C + C]
                    x = x[:, (block % 2) * C : (block % 2) * C + C]
                    out_ref[0, a * 9 + b * 3 + cc] = x
                else:
                    for part in range(2):
                        row = b * C + part * 32
                        side = 0 if row < 96 else 1
                        x = full[768 + row - 96 * side : 768 + row - 96 * side + 32, side * C : side * C + C]
                        out_ref[0, a * 9 + b * 3 + cc, part * 32 : part * 32 + 32] = x


def gather_body(s_ref, x0, x1, x2, x3, out_ref):
    s = s_ref[0]
    for k, ref in enumerate((x0, x1, x2, x3)):
        out_ref[0, (s + N - k) % N] = ref[...]


def shift(x, by):
    return lax.ppermute(x, "section", [(i, (i + by) % N) for i in range(N)])


def handed(parts):
    return [parts[0]] + [shift(parts[k], k) for k in (1, 2, 3)]


def swapped(x):
    return lax.ppermute(x, CORE, [(0, 1), (1, 0)])


def neighbours(to_right, to_left):
    count = lax.axis_size(DEPTH)
    left = lax.ppermute(to_right, DEPTH, [(i, i + 1) for i in range(count - 1)])
    right = lax.ppermute(to_left, DEPTH, [(i + 1, i) for i in range(count - 1)])
    return left, right


def window(activations, filters, cotangent):
    s = lax.axis_index("section")
    c = lax.axis_index(CORE)
    place = jnp.stack([s, c]).astype(jnp.int32)
    act = activations[0]
    plane = (C, H * W)
    two = ((2, *plane), F32)
    three = ((3, *plane), F32)

    left, right = neighbours(act[:, 1], act[:, 0])
    forward, mine, yours = run(
        prepare_body,
        (place, filters),
        [((384, 576), BF16), ((96, 576), F32), ((96, 576), F32)],
        [((192, 576), F32)],
        flops=10**6,
    )
    *factors, vh, vl = run(
        slope_body,
        (place, act, left, right, forward),
        [two] * 4 + [((N, 4, 192, 256), BF16)] * 2,
        flops=2 * 8 * 192 * 576 * 256 * 3,
    )
    factors = handed(factors)

    below = shift(mine, 1)
    above = shift(mine, -1)
    far0 = shift(below[:48], 1)
    far1 = shift(above[48:], -1)
    other = swapped(jnp.concatenate([below, above, far0, far1], axis=0))
    (taps,) = run(
        taps_body, (place, mine, yours, below, above, far0, far1, other), [((N, 384, 576), BF16)], flops=10**6
    )

    s3, to_right, to_left = run(pick_body, (place, *factors, cotangent), [two, three, three], flops=10**6)
    left, right = neighbours(to_right, to_left)
    scratch = [((6, 192, 256), BF16)] * 2 + [((4, 192, 256), BF16)] * 2
    ig3, s2, ig2, s1, to_right, to_left = run(
        top_body,
        (place, left, right, *factors, s3, taps),
        [two, two, two, two, three, three],
        scratch,
        flops=2 * 6 * 192 * 576 * 256 * 3,
    )
    left, right = neighbours(to_right, to_left)
    packed = run(
        low_body,
        (place, left, right, *factors, s3, s2, s1, ig3, ig2, taps),
        [two] * 8,
        [((2, *plane), F32)] * 3 + scratch,
        flops=2 * 6 * 192 * 576 * 256 * 3,
    )
    slopes = handed(packed[:4])
    slopes, grads = lax.optimization_barrier((slopes, packed[4:]))
    grads = handed(grads)

    keep, send = run(
        filter_body,
        (place, *slopes, vh, vl),
        [((512, 128), F32)] * 2,
        [((192, 576), F32)],
        flops=2 * 8 * 192 * 576 * 256 * 3,
    )
    part = (keep + swapped(send)).reshape(32, 16, 128)
    (input_grads,) = run(gather_body, (place, *grads), [((1, N, 2, *plane), F32)], flops=10**6)
    part, input_grads = lax.optimization_barrier((part, input_grads))
    part = lax.all_to_all(part, PLANE, 0, 0, tiled=True)
    scaling = 1.0 / math.sqrt(N * 2 * lax.axis_size(DEPTH) * H * W)
    total = jnp.sum(part, axis=0) * scaling
    part = lax.all_to_all(jnp.broadcast_to(total[None], (32, 16, 128)), PLANE, 0, 0, tiled=True).reshape(512, 128)
    other_part = swapped(part)
    (filter_grads,) = run(
        finish_body, (place, part, other_part), [((1, 27, C, C), F32)], [((864, 128), F32)], flops=10**6
    )
    return input_grads, filter_grads


def solution(mesh):
    finer = Mesh(
        mesh.devices.reshape(mesh.shape["section"], 8, 4, 2),
        ("section", "depth_0", "depth_1", "depth_2"),
    )
    placed = (
        P("section", None, DEPTH, None, None),
        P("section", None, None, None),
        P(None, DEPTH, None, None),
    )
    return jax.shard_map(
        window,
        mesh=finer,
        in_specs=placed,
        out_specs=(P("section", None, DEPTH, None, None), P("section", None, None, None)),
        check_vma=False,
    )
```

```python
import functools
import math

import jax
import jax.numpy as jnp
from jax import lax
from jax.experimental import pallas as pl
from jax.experimental.pallas import tpu as pltpu
from jax.sharding import Mesh
from jax.sharding import PartitionSpec as P


H = 16
W = 16
C = 64
DEPTH = ("depth_0", "depth_1", "depth_2")
PLANE = ("depth_0", "depth_1")
CORE = "depth_2"
N = 4
F32 = jnp.float32
BF16 = jnp.bfloat16
LIMIT = 24 * 2**20
VMEM = pl.BlockSpec(memory_space=pltpu.VMEM)
SMEM = pl.BlockSpec(memory_space=pltpu.SMEM)


def run(body, args, outs, scratch=(), flops=0):
    nbytes = sum(a.size * a.dtype.itemsize for a in args)
    return pl.pallas_call(
        body,
        out_shape=[jax.ShapeDtypeStruct(s, t) for s, t in outs],
        in_specs=[SMEM] + [VMEM] * (len(args) - 1),
        out_specs=[VMEM] * len(outs),
        scratch_shapes=[pltpu.VMEM(s, t) for s, t in scratch],
        cost_estimate=pl.CostEstimate(flops=flops, bytes_accessed=nbytes, transcendentals=0),
        compiler_params=pltpu.CompilerParams(vmem_limit_bytes=LIMIT),
    )(*args)


def split(x):
    high = x.astype(BF16)
    return high, (x - high.astype(F32)).astype(BF16)


def columns():
    return lax.broadcasted_iota(jnp.int32, (C, H * W), 1)


def across(x):
    place = columns()
    left = jnp.where(place % W == 0, 0.0, pltpu.roll(x, 1, 1))
    right = jnp.where(place % W == W - 1, 0.0, pltpu.roll(x, H * W - 1, 1))
    return jnp.concatenate([left, x, right], axis=0)


def down(x):
    return jnp.where(columns() < W, 0.0, pltpu.roll(x, W, 1))


def up(x):
    return jnp.where(columns() >= H * W - W, 0.0, pltpu.roll(x, H * W - W, 1))


def dot(a, b):
    return jnp.dot(a, b, preferred_element_type=F32)


def conv(taps, high, low):
    first = dot(taps, high)
    z = first[:192] + first[192:] + dot(taps[:192], low)
    return z[C : 2 * C] + down(z[:C]) + up(z[2 * C :])


def silu_slope(preact):
    gate = 1.0 / (1.0 + jnp.exp(-preact))
    return gate * (1.0 + preact * (1.0 - gate))


def prepare_body(s_ref, f_ref, forward_ref, mine_ref, yours_ref, back):
    for b in range(3):
        rows = slice(b * C, b * C + C)
        low_rows = slice(192 + b * C, 192 + b * C + C)
        taps = [f_ref[0, a * 9 + b * 3 + cc] for a in range(3) for cc in range(3)]
        high, low = split(jnp.concatenate(taps, axis=1))
        forward_ref[rows] = high
        forward_ref[low_rows] = low
        taps = [f_ref[0, (2 - a) * 9 + (2 - b) * 3 + 2 - cc] for a in range(3) for cc in range(3)]
        back[rows] = jnp.concatenate(taps, axis=0).T
    c = s_ref[1]
    mine_ref[...] = back[pl.ds(pl.multiple_of(c * 96, 32), 96)]
    yours_ref[...] = back[pl.ds(pl.multiple_of((1 - c) * 96, 32), 96)]


def slope_body(ks, s_ref, act_ref, inner_ref, outer_ref, taps_ref, *refs):
    c = s_ref[1]
    for i, k in enumerate(ks):
        m = s_ref[0] ^ k
        out, vh_ref, vl_ref = refs[3 * i : 3 * i + 3]
        for e in range(4):
            if e == 0:
                x = jnp.where(c == 0, outer_ref[m], inner_ref[m])
            elif e == 3:
                x = jnp.where(c == 0, inner_ref[m], outer_ref[m])
            else:
                x = act_ref[m, e - 1]
            high, low = split(across(x))
            vh_ref[e] = high
            vl_ref[e] = low
        for d in range(2):
            z = conv(taps_ref[...], vh_ref[d : d + 3].reshape(576, 256), vl_ref[d : d + 3].reshape(576, 256))
            out[d] = silu_slope(z)


def chosen(index, refs, *at):
    out = refs[0][at]
    for k in range(1, len(refs)):
        out = jnp.where(index == k, refs[k][at], out)
    return out


def ends(c, planes, face_at, inner_ref, outer_ref):
    for d in range(2):
        inner_ref[d] = planes[d]
        outer_ref[d] = planes[d]
    first, last = face_at(0), face_at(1)
    inner_ref[2] = jnp.where(c == 0, last, first)
    outer_ref[2] = jnp.where(c == 0, first, last)


def pick_body(s_ref, d0, d1, d2, d3, cot_ref, s3_ref, inner_ref, outer_ref):
    m = s_ref[0]
    refs = (d0, d1, d2, d3)
    top = [cot_ref[m, d] * chosen(m ^ 3, refs, d) for d in range(2)]
    for d in range(2):
        s3_ref[d] = top[d]
    ends(s_ref[1], top, lambda d: chosen(m ^ 2, refs, d), inner_ref, outer_ref)


def taps_body(s_ref, mine_ref, yours_ref, one_ref, three_ref, far0_ref, far1_ref, other_ref, out_ref):
    s = s_ref[0]
    c = s_ref[1]

    def put(layer, row, x):
        high, low = split(x)
        size = x.shape[0]
        out_ref[layer, pl.ds(row, size)] = high
        out_ref[layer, pl.ds(192 + row, size)] = low

    mine = pl.multiple_of(c * 96, 32)
    yours = pl.multiple_of((1 - c) * 96, 32)
    put(s, mine, mine_ref[...])
    put(s, yours, yours_ref[...])
    put(s ^ 1, mine, one_ref[...])
    put(s ^ 3, mine, three_ref[...])
    put(s ^ 2, mine, jnp.concatenate([far0_ref[...], far1_ref[...]], axis=0))
    put(s ^ 1, yours, other_ref[0:96])
    put(s ^ 3, yours, other_ref[96:192])
    put(s ^ 2, yours, other_ref[192:288])


def upper(layer, s_ref, inner_ref, outer_ref, factors, mid_ref, taps_ref, ig_ref, vh, vl, wh, wl):
    m = s_ref[0]
    c = s_ref[1]

    def left(e):
        return jnp.where(c == 0, outer_ref[e], inner_ref[e])

    def right(e):
        return jnp.where(c == 0, inner_ref[e], outer_ref[e])

    for e in range(6):
        x = left(e) if e < 2 else (mid_ref[e - 2] if e < 4 else right(e - 4))
        high, low = split(across(x))
        vh[e] = high
        vl[e] = low
    slopes = []
    for d in range(4):
        g = conv(taps_ref[layer], vh[d : d + 3].reshape(576, 256), vl[d : d + 3].reshape(576, 256))
        if d == 0:
            factor = left(2)
        elif d == 3:
            factor = right(2)
        else:
            factor = chosen(m ^ (layer - 1), factors, d - 1)
        slope = g * factor
        if 0 < d < 3:
            ig_ref[d - 1] = g
            slopes.append(slope)
        high, low = split(across(slope))
        wh[d] = high
        wl[d] = low
    return slopes


def lower(layer, taps_ref, wh, wl):
    return [conv(taps_ref[layer], wh[d : d + 3].reshape(576, 256), wl[d : d + 3].reshape(576, 256)) for d in range(2)]


def top_body(s_ref, inner_in, outer_in, d0, d1, d2, d3, s3_ref, taps_ref, *refs):
    ig3, s2, ig2, s1, inner_ref, outer_ref, vh, vl, wh, wl = refs
    m = s_ref[0]
    factors = (d0, d1, d2, d3)
    for d, x in enumerate(upper(3, s_ref, inner_in, outer_in, factors, s3_ref, taps_ref, ig3, vh, vl, wh, wl)):
        s2[d] = x
    grads = lower(2, taps_ref, wh, wl)
    slopes = [grads[d] * chosen(m ^ 1, factors, d) for d in range(2)]
    for d in range(2):
        ig2[d] = grads[d]
        s1[d] = slopes[d]
    ends(s_ref[1], slopes, lambda d: chosen(m, factors, d), inner_ref, outer_ref)


def low_body(s_ref, inner_in, outer_in, d0, d1, d2, d3, s3, s2, s1, taps_ref, *refs):
    o, ig1, wh, wl, s0, vh, vl = refs[:4], *refs[4:]
    m = s_ref[0]
    for d, x in enumerate(upper(1, s_ref, inner_in, outer_in, (d0, d1, d2, d3), s1, taps_ref, ig1, vh, vl, wh, wl)):
        s0[d] = x
    for d in range(2):
        for k in range(N):
            o[k][d] = chosen(m ^ k, (s0, s1, s2, s3), d)


def last_body(s_ref, wh, wl, ig3, ig2, ig1, taps_ref, p0, p1, p2, p3, ig0):
    m = s_ref[0]
    for d, g in enumerate(lower(0, taps_ref, wh, wl)):
        ig0[d] = g
    for d in range(2):
        for k, p in enumerate((p0, p1, p2, p3)):
            p[d] = chosen(m ^ k, (ig0, ig1, ig2, ig3), d)


def filter_term(ref, vh_ref, vl_ref):
    nt = (((1,), (1,)), ((), ()))
    total = None
    for d in range(2):
        x = ref[d]
        high, low = split(jnp.concatenate([up(x), x, down(x)], axis=0))
        right_high = vh_ref[d : d + 3].reshape(576, 256)
        right_low = vl_ref[d : d + 3].reshape(576, 256)
        first = lax.dot_general(jnp.concatenate([high, low], axis=0), right_high, nt, preferred_element_type=F32)
        z = first[:192] + first[192:] + lax.dot_general(high, right_low, nt, preferred_element_type=F32)
        total = z if total is None else total + z
    return total


def filter_body(s_ref, *refs):
    keep_ref, send_ref, acc = refs[12:]
    c = s_ref[1]
    for k in range(N):
        term = filter_term(*refs[3 * k : 3 * k + 3])
        acc[...] = term if k == 0 else acc[...] + term

    def piece(row, size):
        if row < 768:
            j = row // 192
            return acc[row - j * 192 : row - j * 192 + size, j * 128 : (j + 1) * 128]
        r = row - 768
        return jnp.concatenate([acc[r : r + size, 512:576], acc[r + 96 : r + 96 + size, 512:576]], axis=1)

    for half in range(2):

        def fill(ref):
            row = 432 * half
            stop = row + 432
            while row < stop:
                size = min((row // 192 + 1) * 192 if row < 768 else 864, stop) - row
                ref[row - 432 * half : row - 432 * half + size] = piece(row, size)
                row += size
            ref[432:512] = jnp.zeros((80, 128), F32)

        @pl.when(c == half)
        def _():
            fill(keep_ref)

        @pl.when(c != half)
        def _():
            fill(send_ref)


def finish_body(s_ref, own_ref, other_ref, out_ref, full):
    c = s_ref[1]
    full[pl.ds(pl.multiple_of(c * 432, 8), 432)] = own_ref[0:432]
    full[pl.ds(pl.multiple_of((1 - c) * 432, 8), 432)] = other_ref[0:432]
    for a in range(3):
        for b in range(3):
            for cc in range(3):
                block = a * 3 + cc
                if block < 8:
                    x = full[(block // 2) * 192 + b * C : (block // 2) * 192 + b * C + C]
                    x = x[:, (block % 2) * C : (block % 2) * C + C]
                    out_ref[0, a * 9 + b * 3 + cc] = x
                else:
                    for part in range(2):
                        row = b * C + part * 32
                        side = 0 if row < 96 else 1
                        x = full[768 + row - 96 * side : 768 + row - 96 * side + 32, side * C : side * C + C]
                        out_ref[0, a * 9 + b * 3 + cc, part * 32 : part * 32 + 32] = x


def gather_body(s_ref, x0, x1, x2, x3, out_ref):
    s = s_ref[0]
    for k, ref in enumerate((x0, x1, x2, x3)):
        out_ref[0, s ^ k] = ref[...]


def met(x, k):
    return lax.ppermute(x, "section", [(i, i ^ k) for i in range(N)])


def handed(parts):
    return [parts[0]] + [met(parts[k], k) for k in (1, 2, 3)]


def swapped(x):
    return lax.ppermute(x, CORE, [(0, 1), (1, 0)])


def neighbours(inner, outer):
    count = lax.axis_size(DEPTH)
    inner = swapped(inner)
    pairs = [(i, i + 1) for i in range(1, count - 1, 2)]
    outer = lax.ppermute(outer, DEPTH, pairs + [(j, i) for i, j in pairs])
    return inner, outer


def window(activations, filters, cotangent):
    s = lax.axis_index("section")
    c = lax.axis_index(CORE)
    place = jnp.stack([s, c]).astype(jnp.int32)
    act = activations[0]
    plane = (C, H * W)
    two = ((2, *plane), F32)
    three = ((3, *plane), F32)

    inner = lax.dynamic_index_in_dim(act, 1 - c, 1, keepdims=False)
    outer = lax.dynamic_index_in_dim(act, c, 1, keepdims=False)
    inner, outer = neighbours(inner, outer)
    forward, mine, yours = run(
        prepare_body,
        (place, filters),
        [((384, 576), BF16), ((96, 576), F32), ((96, 576), F32)],
        [((192, 576), F32)],
        flops=10**6,
    )
    factors, shifted = [None] * N, [None] * N
    for ks in ((2,), (1, 3), (0,)):
        out = run(
            functools.partial(slope_body, ks),
            (place, act, inner, outer, forward),
            [two, ((4, 192, 256), BF16), ((4, 192, 256), BF16)] * len(ks),
            flops=2 * 2 * 192 * 576 * 256 * 3 * len(ks),
        )
        for i, k in enumerate(ks):
            factors[k], *shifted[k] = out[3 * i : 3 * i + 3]
    factors = handed(factors)

    one = met(mine, 1)
    three_half = met(mine, 3)
    far0 = met(three_half[:48], 1)
    far1 = met(one[48:], 3)
    other = swapped(jnp.concatenate([one, three_half, far0, far1], axis=0))
    (taps,) = run(
        taps_body, (place, mine, yours, one, three_half, far0, far1, other), [((N, 384, 576), BF16)], flops=10**6
    )

    s3, inner, outer = run(pick_body, (place, *factors, cotangent), [two, three, three], flops=10**6)
    inner, outer = neighbours(inner, outer)
    scratch = [((6, 192, 256), BF16)] * 2 + [((4, 192, 256), BF16)] * 2
    ig3, s2, ig2, s1, inner, outer = run(
        top_body,
        (place, inner, outer, *factors, s3, taps),
        [two, two, two, two, three, three],
        scratch,
        flops=2 * 6 * 192 * 576 * 256 * 3,
    )
    inner, outer = neighbours(inner, outer)
    *packed, ig1, wh, wl = run(
        low_body,
        (place, inner, outer, *factors, s3, s2, s1, taps),
        [two] * 5 + [((4, 192, 256), BF16)] * 2,
        [((2, *plane), F32)] + scratch[:2],
        flops=2 * 4 * 192 * 576 * 256 * 3,
    )
    slopes = handed(packed)
    packed = run(
        last_body,
        (place, wh, wl, ig3, ig2, ig1, taps),
        [two] * 4,
        [((2, *plane), F32)],
        flops=2 * 2 * 192 * 576 * 256 * 3,
    )
    grads = handed(packed)

    keep, send = run(
        filter_body,
        (place, *(x for k in range(N) for x in (slopes[k], *shifted[k]))),
        [((512, 128), F32)] * 2,
        [((192, 576), F32)],
        flops=2 * 8 * 192 * 576 * 256 * 3,
    )
    part = (keep + swapped(send)).reshape(32, 16, 128)
    part = lax.all_to_all(part, PLANE, 0, 0, tiled=True)
    scaling = 1.0 / math.sqrt(N * 2 * lax.axis_size(DEPTH) * H * W)
    total = jnp.sum(part, axis=0) * scaling
    part = lax.all_to_all(jnp.broadcast_to(total[None], (32, 16, 128)), PLANE, 0, 0, tiled=True).reshape(512, 128)
    other_part = swapped(part)
    (filter_grads,) = run(
        finish_body, (place, part, other_part), [((1, 27, C, C), F32)], [((864, 128), F32)], flops=10**6
    )
    (input_grads,) = run(gather_body, (place, *grads), [((1, N, 2, *plane), F32)], flops=10**6)
    return input_grads, filter_grads


def solution(mesh):
    finer = Mesh(
        mesh.devices.reshape(mesh.shape["section"], 8, 4, 2),
        ("section", "depth_0", "depth_1", "depth_2"),
    )
    placed = (
        P("section", None, DEPTH, None, None),
        P("section", None, None, None),
        P(None, DEPTH, None, None),
    )
    return jax.shard_map(
        window,
        mesh=finer,
        in_specs=placed,
        out_specs=(P("section", None, DEPTH, None, None), P("section", None, None, None)),
        check_vma=False,
    )
```

```python
import functools
import math

import jax
import jax.numpy as jnp
from jax import lax
from jax.experimental import pallas as pl
from jax.experimental.pallas import tpu as pltpu
from jax.sharding import Mesh
from jax.sharding import PartitionSpec as P


H = 16
W = 16
C = 64
DEPTH = ("depth_0", "depth_1", "depth_2")
PLANE = ("depth_0", "depth_1")
CORE = "depth_2"
N = 4
F32 = jnp.float32
BF16 = jnp.bfloat16
LIMIT = 24 * 2**20
VMEM = pl.BlockSpec(memory_space=pltpu.VMEM)


def run(body, args, outs, scratch=(), flops=0):
    nbytes = sum(a.size * a.dtype.itemsize for a in args)
    return pl.pallas_call(
        body,
        out_shape=[jax.ShapeDtypeStruct(s, t) for s, t in outs],
        in_specs=[VMEM] * len(args),
        out_specs=[VMEM] * len(outs),
        scratch_shapes=[pltpu.VMEM(s, t) for s, t in scratch],
        cost_estimate=pl.CostEstimate(flops=flops, bytes_accessed=nbytes, transcendentals=0),
        compiler_params=pltpu.CompilerParams(vmem_limit_bytes=LIMIT),
    )(*args)


def section():
    return lax.axis_index("section")


def core():
    return lax.axis_index(CORE)


def split(x):
    high = x.astype(BF16)
    return high, (x - high.astype(F32)).astype(BF16)


def columns():
    return lax.broadcasted_iota(jnp.int32, (C, H * W), 1)


def across(x):
    place = columns()
    left = jnp.where(place % W == 0, 0.0, pltpu.roll(x, 1, 1))
    right = jnp.where(place % W == W - 1, 0.0, pltpu.roll(x, H * W - 1, 1))
    return jnp.concatenate([left, x, right], axis=0)


def down(x):
    return jnp.where(columns() < W, 0.0, pltpu.roll(x, W, 1))


def up(x):
    return jnp.where(columns() >= H * W - W, 0.0, pltpu.roll(x, H * W - W, 1))


def dot(a, b):
    return jnp.dot(a, b, preferred_element_type=F32)


def conv(taps, high, low):
    first = dot(taps, high)
    z = first[:192] + first[192:] + dot(taps[:192], low)
    return z[C : 2 * C] + down(z[:C]) + up(z[2 * C :])


def silu_slope(preact):
    gate = 1.0 / (1.0 + jnp.exp(-preact))
    return gate * (1.0 + preact * (1.0 - gate))


def prepare_body(f_ref, forward_ref, mine_ref, yours_ref, back):
    for b in range(3):
        rows = slice(b * C, b * C + C)
        low_rows = slice(192 + b * C, 192 + b * C + C)
        taps = [f_ref[0, a * 9 + b * 3 + cc] for a in range(3) for cc in range(3)]
        high, low = split(jnp.concatenate(taps, axis=1))
        forward_ref[rows] = high
        forward_ref[low_rows] = low
        taps = [f_ref[0, (2 - a) * 9 + (2 - b) * 3 + 2 - cc] for a in range(3) for cc in range(3)]
        back[rows] = jnp.concatenate(taps, axis=0).T
    c = core()
    mine_ref[...] = back[pl.ds(pl.multiple_of(c * 96, 32), 96)]
    yours_ref[...] = back[pl.ds(pl.multiple_of((1 - c) * 96, 32), 96)]


def slope_body(ks, act_ref, inner_ref, outer_ref, taps_ref, *refs):
    c = core()
    for i, k in enumerate(ks):
        m = section() ^ k
        out, vh_ref, vl_ref = refs[3 * i : 3 * i + 3]
        for e in range(4):
            if e == 0:
                x = jnp.where(c == 0, outer_ref[m], inner_ref[m])
            elif e == 3:
                x = jnp.where(c == 0, inner_ref[m], outer_ref[m])
            else:
                x = act_ref[m, e - 1]
            high, low = split(across(x))
            vh_ref[e] = high
            vl_ref[e] = low
        for d in range(2):
            z = conv(taps_ref[...], vh_ref[d : d + 3].reshape(576, 256), vl_ref[d : d + 3].reshape(576, 256))
            out[d] = silu_slope(z)


def chosen(index, refs, *at):
    out = refs[0][at]
    for k in range(1, len(refs)):
        out = jnp.where(index == k, refs[k][at], out)
    return out


def ends(c, planes, face_at, inner_ref, outer_ref):
    for d in range(2):
        inner_ref[d] = planes[d]
        outer_ref[d] = planes[d]
    first, last = face_at(0), face_at(1)
    inner_ref[2] = jnp.where(c == 0, last, first)
    outer_ref[2] = jnp.where(c == 0, first, last)


def pick_body(d0, d1, d2, d3, cot_ref, s3_ref, inner_ref, outer_ref):
    m = section()
    refs = (d0, d1, d2, d3)
    top = [cot_ref[m, d] * chosen(m ^ 3, refs, d) for d in range(2)]
    for d in range(2):
        s3_ref[d] = top[d]
    ends(core(), top, lambda d: chosen(m ^ 2, refs, d), inner_ref, outer_ref)


def taps_body(mine_ref, yours_ref, one_ref, three_ref, far0_ref, far1_ref, other_ref, out_ref):
    s = section()
    c = core()

    def put(layer, row, x):
        high, low = split(x)
        size = x.shape[0]
        out_ref[layer, pl.ds(row, size)] = high
        out_ref[layer, pl.ds(192 + row, size)] = low

    mine = pl.multiple_of(c * 96, 32)
    yours = pl.multiple_of((1 - c) * 96, 32)
    put(s, mine, mine_ref[...])
    put(s, yours, yours_ref[...])
    put(s ^ 1, mine, one_ref[...])
    put(s ^ 3, mine, three_ref[...])
    put(s ^ 2, mine, jnp.concatenate([far0_ref[...], far1_ref[...]], axis=0))
    put(s ^ 1, yours, other_ref[0:96])
    put(s ^ 3, yours, other_ref[96:192])
    put(s ^ 2, yours, other_ref[192:288])


def upper(layer, inner_ref, outer_ref, factors, mid_ref, taps_ref, ig_ref, vh, vl, wh, wl):
    m = section()
    c = core()

    def left(e):
        return jnp.where(c == 0, outer_ref[e], inner_ref[e])

    def right(e):
        return jnp.where(c == 0, inner_ref[e], outer_ref[e])

    for e in range(6):
        x = left(e) if e < 2 else (mid_ref[e - 2] if e < 4 else right(e - 4))
        high, low = split(across(x))
        vh[e] = high
        vl[e] = low
    slopes = []
    for d in range(4):
        g = conv(taps_ref[layer], vh[d : d + 3].reshape(576, 256), vl[d : d + 3].reshape(576, 256))
        if d == 0:
            factor = left(2)
        elif d == 3:
            factor = right(2)
        else:
            factor = chosen(m ^ (layer - 1), factors, d - 1)
        slope = g * factor
        if 0 < d < 3:
            ig_ref[d - 1] = g
            slopes.append(slope)
        high, low = split(across(slope))
        wh[d] = high
        wl[d] = low
    return slopes


def lower(layer, taps_ref, wh, wl):
    return [conv(taps_ref[layer], wh[d : d + 3].reshape(576, 256), wl[d : d + 3].reshape(576, 256)) for d in range(2)]


def top_body(inner_in, outer_in, d0, d1, d2, d3, s3_ref, taps_ref, *refs):
    ig3, s2, ig2, s1, inner_ref, outer_ref, vh, vl, wh, wl = refs
    m = section()
    factors = (d0, d1, d2, d3)
    for d, x in enumerate(upper(3, inner_in, outer_in, factors, s3_ref, taps_ref, ig3, vh, vl, wh, wl)):
        s2[d] = x
    grads = lower(2, taps_ref, wh, wl)
    slopes = [grads[d] * chosen(m ^ 1, factors, d) for d in range(2)]
    for d in range(2):
        ig2[d] = grads[d]
        s1[d] = slopes[d]
    ends(core(), slopes, lambda d: chosen(m, factors, d), inner_ref, outer_ref)


def low_body(inner_in, outer_in, d0, d1, d2, d3, s3, s2, s1, taps_ref, *refs):
    o, ig1, wh, wl, s0, vh, vl = refs[:4], *refs[4:]
    m = section()
    for d, x in enumerate(upper(1, inner_in, outer_in, (d0, d1, d2, d3), s1, taps_ref, ig1, vh, vl, wh, wl)):
        s0[d] = x
    for d in range(2):
        for k in range(N):
            o[k][d] = chosen(m ^ k, (s0, s1, s2, s3), d)


def last_body(wh, wl, ig3, ig2, ig1, taps_ref, p0, p1, p2, p3, ig0):
    m = section()
    for d, g in enumerate(lower(0, taps_ref, wh, wl)):
        ig0[d] = g
    for d in range(2):
        for k, p in enumerate((p0, p1, p2, p3)):
            p[d] = chosen(m ^ k, (ig0, ig1, ig2, ig3), d)


def filter_term(ref, vh_ref, vl_ref):
    nt = (((1,), (1,)), ((), ()))
    total = None
    for d in range(2):
        x = ref[d]
        high, low = split(jnp.concatenate([up(x), x, down(x)], axis=0))
        right_high = vh_ref[d : d + 3].reshape(576, 256)
        right_low = vl_ref[d : d + 3].reshape(576, 256)
        first = lax.dot_general(jnp.concatenate([high, low], axis=0), right_high, nt, preferred_element_type=F32)
        z = first[:192] + first[192:] + lax.dot_general(high, right_low, nt, preferred_element_type=F32)
        total = z if total is None else total + z
    return total


def filter_body(*refs):
    keep_ref, send_ref, acc = refs[12:]
    c = core()
    for k in range(N):
        term = filter_term(*refs[3 * k : 3 * k + 3])
        acc[...] = term if k == 0 else acc[...] + term

    def piece(row, size):
        if row < 768:
            j = row // 192
            return acc[row - j * 192 : row - j * 192 + size, j * 128 : (j + 1) * 128]
        r = row - 768
        return jnp.concatenate([acc[r : r + size, 512:576], acc[r + 96 : r + 96 + size, 512:576]], axis=1)

    for half in range(2):

        def fill(ref):
            row = 432 * half
            stop = row + 432
            while row < stop:
                size = min((row // 192 + 1) * 192 if row < 768 else 864, stop) - row
                ref[row - 432 * half : row - 432 * half + size] = piece(row, size)
                row += size
            ref[432:512] = jnp.zeros((80, 128), F32)

        @pl.when(c == half)
        def _():
            fill(keep_ref)

        @pl.when(c != half)
        def _():
            fill(send_ref)


def finish_body(own_ref, other_ref, out_ref, full):
    c = core()
    full[pl.ds(pl.multiple_of(c * 432, 8), 432)] = own_ref[0:432]
    full[pl.ds(pl.multiple_of((1 - c) * 432, 8), 432)] = other_ref[0:432]
    for a in range(3):
        for b in range(3):
            for cc in range(3):
                block = a * 3 + cc
                if block < 8:
                    x = full[(block // 2) * 192 + b * C : (block // 2) * 192 + b * C + C]
                    x = x[:, (block % 2) * C : (block % 2) * C + C]
                    out_ref[0, a * 9 + b * 3 + cc] = x
                else:
                    for part in range(2):
                        row = b * C + part * 32
                        side = 0 if row < 96 else 1
                        x = full[768 + row - 96 * side : 768 + row - 96 * side + 32, side * C : side * C + C]
                        out_ref[0, a * 9 + b * 3 + cc, part * 32 : part * 32 + 32] = x


def gather_body(x0, x1, x2, x3, out_ref):
    s = section()
    for k, ref in enumerate((x0, x1, x2, x3)):
        out_ref[0, s ^ k] = ref[...]


def met(x, k):
    return lax.ppermute(x, "section", [(i, i ^ k) for i in range(N)])


def handed(parts):
    return [parts[0]] + [met(parts[k], k) for k in (1, 2, 3)]


def swapped(x):
    return lax.ppermute(x, CORE, [(0, 1), (1, 0)])


def neighbours(inner, outer):
    count = lax.axis_size(DEPTH)
    inner = swapped(inner)
    pairs = [(i, i + 1) for i in range(1, count - 1, 2)]
    outer = lax.ppermute(outer, DEPTH, pairs + [(j, i) for i, j in pairs])
    return inner, outer


def window(activations, filters, cotangent):
    c = lax.axis_index(CORE)
    act = activations[0]
    plane = (C, H * W)
    two = ((2, *plane), F32)
    three = ((3, *plane), F32)

    inner = lax.dynamic_index_in_dim(act, 1 - c, 1, keepdims=False)
    outer = lax.dynamic_index_in_dim(act, c, 1, keepdims=False)
    inner, outer = neighbours(inner, outer)
    forward, mine, yours = run(
        prepare_body,
        (filters,),
        [((384, 576), BF16), ((96, 576), F32), ((96, 576), F32)],
        [((192, 576), F32)],
        flops=10**6,
    )
    factors, shifted = [None] * N, [None] * N
    for ks in ((2,), (1, 3), (0,)):
        out = run(
            functools.partial(slope_body, ks),
            (act, inner, outer, forward),
            [two, ((4, 192, 256), BF16), ((4, 192, 256), BF16)] * len(ks),
            flops=2 * 2 * 192 * 576 * 256 * 3 * len(ks),
        )
        for i, k in enumerate(ks):
            factors[k], *shifted[k] = out[3 * i : 3 * i + 3]
    factors = handed(factors)

    one = met(mine, 1)
    three_half = met(mine, 3)
    far0 = met(three_half[:48], 1)
    far1 = met(one[48:], 3)
    other = swapped(jnp.concatenate([one, three_half, far0, far1], axis=0))
    (taps,) = run(taps_body, (mine, yours, one, three_half, far0, far1, other), [((N, 384, 576), BF16)], flops=10**6)

    s3, inner, outer = run(pick_body, (*factors, cotangent), [two, three, three], flops=10**6)
    inner, outer = neighbours(inner, outer)
    scratch = [((6, 192, 256), BF16)] * 2 + [((4, 192, 256), BF16)] * 2
    ig3, s2, ig2, s1, inner, outer = run(
        top_body,
        (inner, outer, *factors, s3, taps),
        [two, two, two, two, three, three],
        scratch,
        flops=2 * 6 * 192 * 576 * 256 * 3,
    )
    inner, outer = neighbours(inner, outer)
    *packed, ig1, wh, wl = run(
        low_body,
        (inner, outer, *factors, s3, s2, s1, taps),
        [two] * 5 + [((4, 192, 256), BF16)] * 2,
        [((2, *plane), F32)] + scratch[:2],
        flops=2 * 4 * 192 * 576 * 256 * 3,
    )
    slopes = handed(packed)
    packed = run(
        last_body, (wh, wl, ig3, ig2, ig1, taps), [two] * 4, [((2, *plane), F32)], flops=2 * 2 * 192 * 576 * 256 * 3
    )
    grads = handed(packed)

    keep, send = run(
        filter_body,
        tuple(x for k in range(N) for x in (slopes[k], *shifted[k])),
        [((512, 128), F32)] * 2,
        [((192, 576), F32)],
        flops=2 * 8 * 192 * 576 * 256 * 3,
    )
    part = (keep + swapped(send)).reshape(32, 16, 128)
    part = lax.all_to_all(part, PLANE, 0, 0, tiled=True)
    scaling = 1.0 / math.sqrt(N * 2 * lax.axis_size(DEPTH) * H * W)
    total = jnp.sum(part, axis=0) * scaling
    part = lax.all_to_all(jnp.broadcast_to(total[None], (32, 16, 128)), PLANE, 0, 0, tiled=True).reshape(512, 128)
    other_part = swapped(part)
    (filter_grads,) = run(finish_body, (part, other_part), [((1, 27, C, C), F32)], [((864, 128), F32)], flops=10**6)
    (input_grads,) = run(gather_body, (*grads,), [((1, N, 2, *plane), F32)], flops=10**6)
    return input_grads, filter_grads


def solution(mesh):
    finer = Mesh(
        mesh.devices.reshape(mesh.shape["section"], 8, 4, 2),
        ("section", "depth_0", "depth_1", "depth_2"),
    )
    placed = (
        P("section", None, DEPTH, None, None),
        P("section", None, None, None),
        P(None, DEPTH, None, None),
    )
    return jax.shard_map(
        window,
        mesh=finer,
        in_specs=placed,
        out_specs=(P("section", None, DEPTH, None, None), P("section", None, None, None)),
        check_vma=False,
    )
```

```python
import functools
import math

import jax
import jax.numpy as jnp
from jax import lax
from jax.experimental import pallas as pl
from jax.experimental.pallas import tpu as pltpu
from jax.sharding import Mesh
from jax.sharding import PartitionSpec as P


H = 16
W = 16
C = 64
DEPTH = ("depth_0", "depth_1", "depth_2")
PLANE = ("depth_0", "depth_1")
CORE = "depth_2"
N = 4
F32 = jnp.float32
BF16 = jnp.bfloat16
LIMIT = 24 * 2**20
VMEM = pl.BlockSpec(memory_space=pltpu.VMEM)


def run(body, args, outs, scratch=(), flops=0):
    nbytes = sum(a.size * a.dtype.itemsize for a in args)
    return pl.pallas_call(
        body,
        out_shape=[jax.ShapeDtypeStruct(s, t) for s, t in outs],
        in_specs=[VMEM] * len(args),
        out_specs=[VMEM] * len(outs),
        scratch_shapes=[pltpu.VMEM(s, t) for s, t in scratch],
        cost_estimate=pl.CostEstimate(flops=flops, bytes_accessed=nbytes, transcendentals=0),
        compiler_params=pltpu.CompilerParams(vmem_limit_bytes=LIMIT),
    )(*args)


def section():
    return lax.axis_index("section")


def core():
    return lax.axis_index(CORE)


def split(x):
    high = x.astype(BF16)
    return high, (x - high.astype(F32)).astype(BF16)


def columns():
    return lax.broadcasted_iota(jnp.int32, (C, H * W), 1)


def across(x):
    place = columns()
    left = jnp.where(place % W == 0, 0.0, pltpu.roll(x, 1, 1))
    right = jnp.where(place % W == W - 1, 0.0, pltpu.roll(x, H * W - 1, 1))
    return jnp.concatenate([left, x, right], axis=0)


def down(x):
    return jnp.where(columns() < W, 0.0, pltpu.roll(x, W, 1))


def up(x):
    return jnp.where(columns() >= H * W - W, 0.0, pltpu.roll(x, H * W - W, 1))


def dot(a, b):
    return jnp.dot(a, b, preferred_element_type=F32)


def conv(taps, high, low):
    first = dot(taps, high)
    z = first[:192] + first[192:] + dot(taps[:192], low)
    return z[C : 2 * C] + down(z[:C]) + up(z[2 * C :])


def silu_slope(preact):
    gate = 1.0 / (1.0 + jnp.exp(-preact))
    return gate * (1.0 + preact * (1.0 - gate))


def prepare_body(f_ref, forward_ref, mine_ref, yours_ref, back):
    for b in range(3):
        rows = slice(b * C, b * C + C)
        low_rows = slice(192 + b * C, 192 + b * C + C)
        taps = [f_ref[0, a * 9 + b * 3 + cc] for a in range(3) for cc in range(3)]
        high, low = split(jnp.concatenate(taps, axis=1))
        forward_ref[rows] = high
        forward_ref[low_rows] = low
        taps = [f_ref[0, (2 - a) * 9 + (2 - b) * 3 + 2 - cc] for a in range(3) for cc in range(3)]
        back[rows] = jnp.concatenate(taps, axis=0).T
    c = core()
    mine_ref[...] = back[pl.ds(pl.multiple_of(c * 96, 32), 96)]
    yours_ref[...] = back[pl.ds(pl.multiple_of((1 - c) * 96, 32), 96)]


def slope_body(ks, act_ref, inner_ref, outer_ref, taps_ref, *refs):
    c = core()
    for i, k in enumerate(ks):
        m = section() ^ k
        out, vh_ref, vl_ref = refs[3 * i : 3 * i + 3]
        for e in range(4):
            if e == 0:
                x = jnp.where(c == 0, outer_ref[m], inner_ref[m])
            elif e == 3:
                x = jnp.where(c == 0, inner_ref[m], outer_ref[m])
            else:
                x = act_ref[m, e - 1]
            high, low = split(across(x))
            vh_ref[e] = high
            vl_ref[e] = low
        for d in range(2):
            z = conv(taps_ref[...], vh_ref[d : d + 3].reshape(576, 256), vl_ref[d : d + 3].reshape(576, 256))
            out[d] = silu_slope(z)


def chosen(index, refs, *at):
    out = refs[0][at]
    for k in range(1, len(refs)):
        out = jnp.where(index == k, refs[k][at], out)
    return out


def by_core(even, odd):
    return jnp.where(core() == 0, even, odd)


def pick_body(d0, d1, d2, d3, cot_ref, s3_ref, inner_ref, outer_ref, one_ref, two_ref):
    m = section()
    refs = (d0, d1, d2, d3)
    top = [cot_ref[m, d] * chosen(m ^ 3, refs, d) for d in range(2)]
    face = [chosen(m ^ 1, refs, d) for d in range(2)]
    for d in range(2):
        s3_ref[d] = top[d]
        below = chosen(m ^ 2, refs, d)
        for ref in (inner_ref, outer_ref):
            ref[d] = top[d]
            ref[2 + d] = below
    inner_ref[4] = by_core(face[1], face[0])
    outer_ref[4] = by_core(face[0], face[1])
    even = lax.rem(lax.axis_index("depth_1"), 2) == 0
    one_ref[0] = jnp.where(even, top[1], top[0])
    two_ref[0] = jnp.where(even, top[0], top[1])


def taps_body(mine_ref, yours_ref, one_ref, three_ref, far0_ref, far1_ref, other_ref, out_ref):
    s = section()
    c = core()

    def put(layer, row, x):
        high, low = split(x)
        size = x.shape[0]
        out_ref[layer, pl.ds(row, size)] = high
        out_ref[layer, pl.ds(192 + row, size)] = low

    mine = pl.multiple_of(c * 96, 32)
    yours = pl.multiple_of((1 - c) * 96, 32)
    put(s, mine, mine_ref[...])
    put(s, yours, yours_ref[...])
    put(s ^ 1, mine, one_ref[...])
    put(s ^ 3, mine, three_ref[...])
    put(s ^ 2, mine, jnp.concatenate([far0_ref[...], far1_ref[...]], axis=0))
    put(s ^ 1, yours, other_ref[0:96])
    put(s ^ 3, yours, other_ref[96:192])
    put(s ^ 2, yours, other_ref[192:288])


def store(x, high_ref, low_ref, at):
    high, low = split(across(x))
    high_ref[at] = high
    low_ref[at] = low


def convs(taps_ref, layer, high_ref, low_ref, count):
    return [
        conv(taps_ref[layer], high_ref[d : d + 3].reshape(576, 256), low_ref[d : d + 3].reshape(576, 256))
        for d in range(count)
    ]


def chain_body(inner_in, outer_in, one_in, two_in, d0, d1, d2, d3, s3, taps_ref, *refs):
    o, ig3, ig2, ig1, s0, inner_ref, outer_ref, s2, s1, ah, al, bh, bl, ch, cl = refs[:4], *refs[4:]
    m = section()
    factors = (d0, d1, d2, d3)
    even = lax.rem(lax.axis_index("depth_1"), 2) == 0

    def left(e):
        return by_core(outer_in[e], inner_in[e])

    def right(e):
        return by_core(inner_in[e], outer_in[e])

    planes = [jnp.where(even, two_in[0], one_in[0]), left(0), left(1), s3[0], s3[1]]
    planes += [right(0), right(1), jnp.where(even, one_in[0], two_in[0])]
    for e, x in enumerate(planes):
        store(x, ah, al, e)
    for e, g in enumerate(convs(taps_ref, 3, ah, al, 6)):
        if e < 2:
            slope = g * left(2 + e)
        elif e > 3:
            slope = g * right(e - 2)
        else:
            slope = g * chosen(m ^ 2, factors, e - 2)
            ig3[e - 2] = g
            s2[e - 2] = slope
        store(slope, bh, bl, e)
    for e, g in enumerate(convs(taps_ref, 2, bh, bl, 4)):
        if e == 0:
            slope = g * left(4)
        elif e == 3:
            slope = g * right(4)
        else:
            slope = g * chosen(m ^ 1, factors, e - 1)
            ig2[e - 1] = g
            s1[e - 1] = slope
        store(slope, ch, cl, e)
    for d, g in enumerate(convs(taps_ref, 1, ch, cl, 2)):
        ig1[d] = g
        s0[d] = g * chosen(m, factors, d)
    for d in range(2):
        for k in range(N):
            o[k][d] = chosen(m ^ k, (s0, s1, s2, s3), d)
    inner_ref[0] = by_core(s0[1], s0[0])
    outer_ref[0] = by_core(s0[0], s0[1])


def last_body(inner_in, outer_in, s0, ig3, ig2, ig1, taps_ref, p0, p1, p2, p3, ig0, vh, vl):
    m = section()
    for e, x in enumerate((by_core(outer_in[0], inner_in[0]), s0[0], s0[1], by_core(inner_in[0], outer_in[0]))):
        store(x, vh, vl, e)
    for d, g in enumerate(convs(taps_ref, 0, vh, vl, 2)):
        ig0[d] = g
    for d in range(2):
        for k, p in enumerate((p0, p1, p2, p3)):
            p[d] = chosen(m ^ k, (ig0, ig1, ig2, ig3), d)


def filter_term(ref, vh_ref, vl_ref):
    nt = (((1,), (1,)), ((), ()))
    total = None
    for d in range(2):
        x = ref[d]
        high, low = split(jnp.concatenate([up(x), x, down(x)], axis=0))
        right_high = vh_ref[d : d + 3].reshape(576, 256)
        right_low = vl_ref[d : d + 3].reshape(576, 256)
        first = lax.dot_general(jnp.concatenate([high, low], axis=0), right_high, nt, preferred_element_type=F32)
        z = first[:192] + first[192:] + lax.dot_general(high, right_low, nt, preferred_element_type=F32)
        total = z if total is None else total + z
    return total


def filter_body(*refs):
    keep_ref, send_ref, acc = refs[12:]
    c = core()
    for k in range(N):
        term = filter_term(*refs[3 * k : 3 * k + 3])
        acc[...] = term if k == 0 else acc[...] + term

    def piece(row, size):
        if row < 768:
            j = row // 192
            return acc[row - j * 192 : row - j * 192 + size, j * 128 : (j + 1) * 128]
        r = row - 768
        return jnp.concatenate([acc[r : r + size, 512:576], acc[r + 96 : r + 96 + size, 512:576]], axis=1)

    for half in range(2):

        def fill(ref):
            row = 432 * half
            stop = row + 432
            while row < stop:
                size = min((row // 192 + 1) * 192 if row < 768 else 864, stop) - row
                ref[row - 432 * half : row - 432 * half + size] = piece(row, size)
                row += size
            ref[432:512] = jnp.zeros((80, 128), F32)

        @pl.when(c == half)
        def _():
            fill(keep_ref)

        @pl.when(c != half)
        def _():
            fill(send_ref)


def finish_body(own_ref, other_ref, out_ref, full):
    c = core()
    full[pl.ds(pl.multiple_of(c * 432, 8), 432)] = own_ref[0:432]
    full[pl.ds(pl.multiple_of((1 - c) * 432, 8), 432)] = other_ref[0:432]
    for a in range(3):
        for b in range(3):
            for cc in range(3):
                block = a * 3 + cc
                if block < 8:
                    x = full[(block // 2) * 192 + b * C : (block // 2) * 192 + b * C + C]
                    x = x[:, (block % 2) * C : (block % 2) * C + C]
                    out_ref[0, a * 9 + b * 3 + cc] = x
                else:
                    for part in range(2):
                        row = b * C + part * 32
                        side = 0 if row < 96 else 1
                        x = full[768 + row - 96 * side : 768 + row - 96 * side + 32, side * C : side * C + C]
                        out_ref[0, a * 9 + b * 3 + cc, part * 32 : part * 32 + 32] = x


def gather_body(x0, x1, x2, x3, out_ref):
    s = section()
    for k, ref in enumerate((x0, x1, x2, x3)):
        out_ref[0, s ^ k] = ref[...]


def met(x, k):
    return lax.ppermute(x, "section", [(i, i ^ k) for i in range(N)])


def handed(parts):
    return [parts[0]] + [met(parts[k], k) for k in (1, 2, 3)]


def swapped(x):
    return lax.ppermute(x, CORE, [(0, 1), (1, 0)])


def neighbours(inner, outer):
    count = lax.axis_size(DEPTH)
    inner = swapped(inner)
    pairs = [(i, i + 1) for i in range(1, count - 1, 2)]
    outer = lax.ppermute(outer, DEPTH, pairs + [(j, i) for i, j in pairs])
    return inner, outer


def skipped(one, two):
    count = lax.axis_size(DEPTH)
    out = []
    for x, first in ((one, 0), (two, 2)):
        pairs = [(i + c, i + c + 2) for i in range(first, count - 2, 4) for c in range(2)]
        out.append(lax.ppermute(x, DEPTH, pairs + [(j, i) for i, j in pairs]))
    return out


def window(activations, filters, cotangent):
    c = lax.axis_index(CORE)
    act = activations[0]
    plane = (C, H * W)
    two = ((2, *plane), F32)

    inner = lax.dynamic_index_in_dim(act, 1 - c, 1, keepdims=False)
    outer = lax.dynamic_index_in_dim(act, c, 1, keepdims=False)
    inner, outer = neighbours(inner, outer)
    forward, mine, yours = run(
        prepare_body,
        (filters,),
        [((384, 576), BF16), ((96, 576), F32), ((96, 576), F32)],
        [((192, 576), F32)],
        flops=10**6,
    )
    factors, shifted = [None] * N, [None] * N
    for ks in ((2,), (1, 3), (0,)):
        out = run(
            functools.partial(slope_body, ks),
            (act, inner, outer, forward),
            [two, ((4, 192, 256), BF16), ((4, 192, 256), BF16)] * len(ks),
            flops=2 * 2 * 192 * 576 * 256 * 3 * len(ks),
        )
        for i, k in enumerate(ks):
            factors[k], *shifted[k] = out[3 * i : 3 * i + 3]
    factors = handed(factors)

    one = met(mine, 1)
    three_half = met(mine, 3)
    far0 = met(three_half[:48], 1)
    far1 = met(one[48:], 3)
    other = swapped(jnp.concatenate([one, three_half, far0, far1], axis=0))
    (taps,) = run(taps_body, (mine, yours, one, three_half, far0, far1, other), [((N, 384, 576), BF16)], flops=10**6)

    one_plane = ((1, *plane), F32)
    five = ((5, *plane), F32)
    s3, inner, outer, one, two_apart = run(
        pick_body, (*factors, cotangent), [two, five, five, one_plane, one_plane], flops=10**6
    )
    inner, outer = neighbours(inner, outer)
    one, two_apart = skipped(one, two_apart)
    shifted_planes = [((e, 192, 256), BF16) for e in (8, 8, 6, 6, 4, 4)]
    *packed, ig3, ig2, ig1, s0, inner, outer = run(
        chain_body,
        (inner, outer, one, two_apart, *factors, s3, taps),
        [two] * 8 + [one_plane] * 2,
        [((2, *plane), F32)] * 2 + shifted_planes,
        flops=2 * 12 * 192 * 576 * 256 * 3,
    )
    slopes = handed(packed)
    inner, outer = neighbours(inner, outer)
    packed = run(
        last_body,
        (inner, outer, s0, ig3, ig2, ig1, taps),
        [two] * 4,
        [((2, *plane), F32)] + shifted_planes[4:],
        flops=2 * 2 * 192 * 576 * 256 * 3,
    )
    grads = handed(packed)

    keep, send = run(
        filter_body,
        tuple(x for k in range(N) for x in (slopes[k], *shifted[k])),
        [((512, 128), F32)] * 2,
        [((192, 576), F32)],
        flops=2 * 8 * 192 * 576 * 256 * 3,
    )
    part = (keep + swapped(send)).reshape(32, 16, 128)
    part = lax.all_to_all(part, PLANE, 0, 0, tiled=True)
    scaling = 1.0 / math.sqrt(N * 2 * lax.axis_size(DEPTH) * H * W)
    total = jnp.sum(part, axis=0) * scaling
    part = lax.all_to_all(jnp.broadcast_to(total[None], (32, 16, 128)), PLANE, 0, 0, tiled=True)
    part = part.reshape(512, 128)
    other_part = swapped(part)
    (filter_grads,) = run(finish_body, (part, other_part), [((1, 27, C, C), F32)], [((864, 128), F32)], flops=10**6)
    (input_grads,) = run(gather_body, (*grads,), [((1, N, 2, *plane), F32)], flops=10**6)
    return input_grads, filter_grads


def solution(mesh):
    finer = Mesh(
        mesh.devices.reshape(mesh.shape["section"], 8, 4, 2),
        ("section", "depth_0", "depth_1", "depth_2"),
    )
    placed = (
        P("section", None, DEPTH, None, None),
        P("section", None, None, None),
        P(None, DEPTH, None, None),
    )
    return jax.shard_map(
        window,
        mesh=finer,
        in_specs=placed,
        out_specs=(P("section", None, DEPTH, None, None), P("section", None, None, None)),
        check_vma=False,
    )
```

```python
import functools
import math

import jax
import jax.numpy as jnp
from jax import lax
from jax.experimental import pallas as pl
from jax.experimental.pallas import tpu as pltpu
from jax.sharding import Mesh
from jax.sharding import PartitionSpec as P


H = 16
W = 16
C = 64
DEPTH = ("depth_0", "depth_1", "depth_2")
PLANE = ("depth_0", "depth_1")
CORE = "depth_2"
N = 4
F32 = jnp.float32
BF16 = jnp.bfloat16
LIMIT = 24 * 2**20
VMEM = pl.BlockSpec(memory_space=pltpu.VMEM)


def run(body, args, outs, scratch=(), flops=0):
    nbytes = sum(a.size * a.dtype.itemsize for a in args)
    return pl.pallas_call(
        body,
        out_shape=[jax.ShapeDtypeStruct(s, t) for s, t in outs],
        in_specs=[VMEM] * len(args),
        out_specs=[VMEM] * len(outs),
        scratch_shapes=[pltpu.VMEM(s, t) for s, t in scratch],
        cost_estimate=pl.CostEstimate(flops=flops, bytes_accessed=nbytes, transcendentals=0),
        compiler_params=pltpu.CompilerParams(vmem_limit_bytes=LIMIT),
    )(*args)


def section():
    return lax.axis_index("section")


def core():
    return lax.axis_index(CORE)


def split(x):
    high = x.astype(BF16)
    return high, (x - high.astype(F32)).astype(BF16)


def columns():
    return lax.broadcasted_iota(jnp.int32, (C, H * W), 1)


def across(x):
    place = columns()
    left = jnp.where(place % W == 0, 0.0, pltpu.roll(x, 1, 1))
    right = jnp.where(place % W == W - 1, 0.0, pltpu.roll(x, H * W - 1, 1))
    return jnp.concatenate([left, x, right], axis=0)


def down(x):
    return jnp.where(columns() < W, 0.0, pltpu.roll(x, W, 1))


def up(x):
    return jnp.where(columns() >= H * W - W, 0.0, pltpu.roll(x, H * W - W, 1))


def dot(a, b):
    return jnp.dot(a, b, preferred_element_type=F32)


def conv(taps, high, low):
    first = dot(taps, high)
    z = first[:192] + first[192:] + dot(taps[:192], low)
    return z[C : 2 * C] + down(z[:C]) + up(z[2 * C :])


def silu_slope(preact):
    gate = 1.0 / (1.0 + jnp.exp(-preact))
    return gate * (1.0 + preact * (1.0 - gate))


def prepare_body(f_ref, forward_ref, mine_ref, yours_ref, back):
    for b in range(3):
        rows = slice(b * C, b * C + C)
        low_rows = slice(192 + b * C, 192 + b * C + C)
        taps = [f_ref[0, a * 9 + b * 3 + cc] for a in range(3) for cc in range(3)]
        high, low = split(jnp.concatenate(taps, axis=1))
        forward_ref[rows] = high
        forward_ref[low_rows] = low
        taps = [f_ref[0, (2 - a) * 9 + (2 - b) * 3 + 2 - cc] for a in range(3) for cc in range(3)]
        back[rows] = jnp.concatenate(taps, axis=0).T
    c = core()
    mine_ref[...] = back[pl.ds(pl.multiple_of(c * 96, 32), 96)]
    yours_ref[...] = back[pl.ds(pl.multiple_of((1 - c) * 96, 32), 96)]


def slope_body(ks, act_ref, inner_ref, outer_ref, taps_ref, *refs):
    c = core()
    for i, k in enumerate(ks):
        m = section() ^ k
        out, vh_ref, vl_ref = refs[3 * i : 3 * i + 3]
        for e in range(4):
            if e == 0:
                x = jnp.where(c == 0, outer_ref[m], inner_ref[m])
            elif e == 3:
                x = jnp.where(c == 0, inner_ref[m], outer_ref[m])
            else:
                x = act_ref[m, e - 1]
            high, low = split(across(x))
            vh_ref[e] = high
            vl_ref[e] = low
        for d in range(2):
            z = conv(taps_ref[...], vh_ref[d : d + 3].reshape(576, 256), vl_ref[d : d + 3].reshape(576, 256))
            out[d] = silu_slope(z)


def chosen(index, refs, *at):
    out = refs[0][at]
    for k in range(1, len(refs)):
        out = jnp.where(index == k, refs[k][at], out)
    return out


def by_core(even, odd):
    return jnp.where(core() == 0, even, odd)


def pick_body(d0, d1, d2, d3, cot_ref, s3_ref, inner_ref, outer_ref, one_ref, two_ref):
    m = section()
    refs = (d0, d1, d2, d3)
    top = [cot_ref[m, d] * chosen(m ^ 3, refs, d) for d in range(2)]
    face = [chosen(m ^ 1, refs, d) for d in range(2)]
    for d in range(2):
        s3_ref[d] = top[d]
        below = chosen(m ^ 2, refs, d)
        for ref in (inner_ref, outer_ref):
            ref[d] = top[d]
            ref[2 + d] = below
    inner_ref[4] = by_core(face[1], face[0])
    outer_ref[4] = by_core(face[0], face[1])
    even = lax.rem(lax.axis_index("depth_1"), 2) == 0
    one_ref[0] = jnp.where(even, top[1], top[0])
    two_ref[0] = jnp.where(even, top[0], top[1])


def taps_body(mine_ref, yours_ref, one_ref, three_ref, far0_ref, far1_ref, other_ref, out_ref):
    s = section()
    c = core()

    def put(layer, row, x):
        high, low = split(x)
        size = x.shape[0]
        out_ref[layer, pl.ds(row, size)] = high
        out_ref[layer, pl.ds(192 + row, size)] = low

    mine = pl.multiple_of(c * 96, 32)
    yours = pl.multiple_of((1 - c) * 96, 32)
    put(s, mine, mine_ref[...])
    put(s, yours, yours_ref[...])
    put(s ^ 1, mine, one_ref[...])
    put(s ^ 3, mine, three_ref[...])
    put(s ^ 2, mine, jnp.concatenate([far0_ref[...], far1_ref[...]], axis=0))
    put(s ^ 1, yours, other_ref[0:96])
    put(s ^ 3, yours, other_ref[96:192])
    put(s ^ 2, yours, other_ref[192:288])


def store(x, high_ref, low_ref, at):
    high, low = split(across(x))
    high_ref[at] = high
    low_ref[at] = low


def convs(taps_ref, layer, high_ref, low_ref, count):
    return [
        conv(taps_ref[layer], high_ref[d : d + 3].reshape(576, 256), low_ref[d : d + 3].reshape(576, 256))
        for d in range(count)
    ]


def chain_body(inner_in, outer_in, one_in, two_in, d0, d1, d2, d3, s3, taps_ref, *refs):
    o, ig3, ig2, ig1, s0, inner_ref, outer_ref, s2, s1, ah, al, bh, bl, ch, cl = refs[:4], *refs[4:]
    m = section()
    factors = (d0, d1, d2, d3)
    even = lax.rem(lax.axis_index("depth_1"), 2) == 0

    def left(e):
        return by_core(outer_in[e], inner_in[e])

    def right(e):
        return by_core(inner_in[e], outer_in[e])

    planes = [jnp.where(even, two_in[0], one_in[0]), left(0), left(1), s3[0], s3[1]]
    planes += [right(0), right(1), jnp.where(even, one_in[0], two_in[0])]
    for e, x in enumerate(planes):
        store(x, ah, al, e)
    for e, g in enumerate(convs(taps_ref, 3, ah, al, 6)):
        if e < 2:
            slope = g * left(2 + e)
        elif e > 3:
            slope = g * right(e - 2)
        else:
            slope = g * chosen(m ^ 2, factors, e - 2)
            ig3[e - 2] = g
            s2[e - 2] = slope
        store(slope, bh, bl, e)
    for e, g in enumerate(convs(taps_ref, 2, bh, bl, 4)):
        if e == 0:
            slope = g * left(4)
        elif e == 3:
            slope = g * right(4)
        else:
            slope = g * chosen(m ^ 1, factors, e - 1)
            ig2[e - 1] = g
            s1[e - 1] = slope
        store(slope, ch, cl, e)
    for d, g in enumerate(convs(taps_ref, 1, ch, cl, 2)):
        ig1[d] = g
        s0[d] = g * chosen(m, factors, d)
    for d in range(2):
        for k in range(N):
            o[k][d] = chosen(m ^ k, (s0, s1, s2, s3), d)
    inner_ref[0] = by_core(s0[1], s0[0])
    outer_ref[0] = by_core(s0[0], s0[1])


def last_body(inner_in, outer_in, s0, ig3, ig2, ig1, taps_ref, p0, p1, p2, p3, ig0, vh, vl):
    m = section()
    for e, x in enumerate((by_core(outer_in[0], inner_in[0]), s0[0], s0[1], by_core(inner_in[0], outer_in[0]))):
        store(x, vh, vl, e)
    for d, g in enumerate(convs(taps_ref, 0, vh, vl, 2)):
        ig0[d] = g
    for d in range(2):
        for k, p in enumerate((p0, p1, p2, p3)):
            p[d] = chosen(m ^ k, (ig0, ig1, ig2, ig3), d)


def filter_body(*refs):
    keep_ref, send_ref, acc = refs[12:]
    c = core()
    nt = (((1,), (1,)), ((), ()))
    both, high_only, right_high, right_low = [], [], [], []
    for k in range(N):
        ref, vh_ref, vl_ref = refs[3 * k : 3 * k + 3]
        for d in range(2):
            x = ref[d]
            high, low = split(jnp.concatenate([up(x), x, down(x)], axis=0))
            both.append(jnp.concatenate([high, low], axis=0))
            high_only.append(high)
            right_high.append(vh_ref[d : d + 3].reshape(576, 256))
            right_low.append(vl_ref[d : d + 3].reshape(576, 256))
    first = lax.dot_general(
        jnp.concatenate(both, axis=1), jnp.concatenate(right_high, axis=1), nt, preferred_element_type=F32
    )
    second = lax.dot_general(
        jnp.concatenate(high_only, axis=1), jnp.concatenate(right_low, axis=1), nt, preferred_element_type=F32
    )
    acc[...] = first[:192] + first[192:] + second

    def piece(row, size):
        if row < 768:
            j = row // 192
            return acc[row - j * 192 : row - j * 192 + size, j * 128 : (j + 1) * 128]
        r = row - 768
        return jnp.concatenate([acc[r : r + size, 512:576], acc[r + 96 : r + 96 + size, 512:576]], axis=1)

    for half in range(2):

        def fill(ref):
            row = 432 * half
            stop = row + 432
            while row < stop:
                size = min((row // 192 + 1) * 192 if row < 768 else 864, stop) - row
                ref[row - 432 * half : row - 432 * half + size] = piece(row, size)
                row += size
            ref[432:512] = jnp.zeros((80, 128), F32)

        @pl.when(c == half)
        def _():
            fill(keep_ref)

        @pl.when(c != half)
        def _():
            fill(send_ref)


def finish_body(own_ref, other_ref, out_ref, full):
    c = core()
    full[pl.ds(pl.multiple_of(c * 432, 8), 432)] = own_ref[0:432]
    full[pl.ds(pl.multiple_of((1 - c) * 432, 8), 432)] = other_ref[0:432]
    for a in range(3):
        for b in range(3):
            for cc in range(3):
                block = a * 3 + cc
                if block < 8:
                    x = full[(block // 2) * 192 + b * C : (block // 2) * 192 + b * C + C]
                    x = x[:, (block % 2) * C : (block % 2) * C + C]
                    out_ref[0, a * 9 + b * 3 + cc] = x
                else:
                    for part in range(2):
                        row = b * C + part * 32
                        side = 0 if row < 96 else 1
                        x = full[768 + row - 96 * side : 768 + row - 96 * side + 32, side * C : side * C + C]
                        out_ref[0, a * 9 + b * 3 + cc, part * 32 : part * 32 + 32] = x


def gather_body(x0, x1, x2, x3, out_ref):
    s = section()
    for k, ref in enumerate((x0, x1, x2, x3)):
        out_ref[0, s ^ k] = ref[...]


def met(x, k):
    return lax.ppermute(x, "section", [(i, i ^ k) for i in range(N)])


def handed(parts):
    return [parts[0]] + [met(parts[k], k) for k in (1, 2, 3)]


def swapped(x):
    return lax.ppermute(x, CORE, [(0, 1), (1, 0)])


def neighbours(inner, outer):
    count = lax.axis_size(DEPTH)
    inner = swapped(inner)
    pairs = [(i, i + 1) for i in range(1, count - 1, 2)]
    outer = lax.ppermute(outer, DEPTH, pairs + [(j, i) for i, j in pairs])
    return inner, outer


def skipped(one, two):
    count = lax.axis_size(DEPTH)
    out = []
    for x, first in ((one, 0), (two, 2)):
        pairs = [(i + c, i + c + 2) for i in range(first, count - 2, 4) for c in range(2)]
        out.append(lax.ppermute(x, DEPTH, pairs + [(j, i) for i, j in pairs]))
    return out


def window(activations, filters, cotangent):
    c = lax.axis_index(CORE)
    act = activations[0]
    plane = (C, H * W)
    two = ((2, *plane), F32)

    inner = lax.dynamic_index_in_dim(act, 1 - c, 1, keepdims=False)
    outer = lax.dynamic_index_in_dim(act, c, 1, keepdims=False)
    inner, outer = neighbours(inner, outer)
    forward, mine, yours = run(
        prepare_body,
        (filters,),
        [((384, 576), BF16), ((96, 576), F32), ((96, 576), F32)],
        [((192, 576), F32)],
        flops=10**6,
    )
    factors, shifted = [None] * N, [None] * N
    for ks in ((2,), (1, 3), (0,)):
        out = run(
            functools.partial(slope_body, ks),
            (act, inner, outer, forward),
            [two, ((4, 192, 256), BF16), ((4, 192, 256), BF16)] * len(ks),
            flops=2 * 2 * 192 * 576 * 256 * 3 * len(ks),
        )
        for i, k in enumerate(ks):
            factors[k], *shifted[k] = out[3 * i : 3 * i + 3]
    factors = handed(factors)

    one = met(mine, 1)
    three_half = met(mine, 3)
    far0 = met(three_half[:48], 1)
    far1 = met(one[48:], 3)
    other = swapped(jnp.concatenate([one, three_half, far0, far1], axis=0))
    (taps,) = run(taps_body, (mine, yours, one, three_half, far0, far1, other), [((N, 384, 576), BF16)], flops=10**6)

    one_plane = ((1, *plane), F32)
    five = ((5, *plane), F32)
    s3, inner, outer, one, two_apart = run(
        pick_body, (*factors, cotangent), [two, five, five, one_plane, one_plane], flops=10**6
    )
    inner, outer = neighbours(inner, outer)
    one, two_apart = skipped(one, two_apart)
    shifted_planes = [((e, 192, 256), BF16) for e in (8, 8, 6, 6, 4, 4)]
    *packed, ig3, ig2, ig1, s0, inner, outer = run(
        chain_body,
        (inner, outer, one, two_apart, *factors, s3, taps),
        [two] * 8 + [one_plane] * 2,
        [((2, *plane), F32)] * 2 + shifted_planes,
        flops=2 * 12 * 192 * 576 * 256 * 3,
    )
    slopes = handed(packed)
    inner, outer = neighbours(inner, outer)
    packed = run(
        last_body,
        (inner, outer, s0, ig3, ig2, ig1, taps),
        [two] * 4,
        [((2, *plane), F32)] + shifted_planes[4:],
        flops=2 * 2 * 192 * 576 * 256 * 3,
    )
    grads = handed(packed)

    keep, send = run(
        filter_body,
        tuple(x for k in range(N) for x in (slopes[k], *shifted[k])),
        [((512, 128), F32)] * 2,
        [((192, 576), F32)],
        flops=2 * 8 * 192 * 576 * 256 * 3,
    )
    part = (keep + swapped(send)).reshape(32, 16, 128)
    part = lax.all_to_all(part, PLANE, 0, 0, tiled=True)
    scaling = 1.0 / math.sqrt(N * 2 * lax.axis_size(DEPTH) * H * W)
    total = jnp.sum(part, axis=0) * scaling
    part = lax.all_to_all(jnp.broadcast_to(total[None], (32, 16, 128)), PLANE, 0, 0, tiled=True)
    part = part.reshape(512, 128)
    other_part = swapped(part)
    (filter_grads,) = run(finish_body, (part, other_part), [((1, 27, C, C), F32)], [((864, 128), F32)], flops=10**6)
    (input_grads,) = run(gather_body, (*grads,), [((1, N, 2, *plane), F32)], flops=10**6)
    return input_grads, filter_grads


def solution(mesh):
    finer = Mesh(
        mesh.devices.reshape(mesh.shape["section"], 8, 4, 2),
        ("section", "depth_0", "depth_1", "depth_2"),
    )
    placed = (
        P("section", None, DEPTH, None, None),
        P("section", None, None, None),
        P(None, DEPTH, None, None),
    )
    return jax.shard_map(
        window,
        mesh=finer,
        in_specs=placed,
        out_specs=(P("section", None, DEPTH, None, None), P("section", None, None, None)),
        check_vma=False,
    )
```

```python
import functools
import math

import jax
import jax.numpy as jnp
from jax import lax
from jax.experimental import pallas as pl
from jax.experimental.pallas import tpu as pltpu
from jax.sharding import Mesh
from jax.sharding import PartitionSpec as P


H = 16
W = 16
C = 64
DEPTH = ("depth_0", "depth_1", "depth_2")
PLANE = ("depth_0", "depth_1")
CORE = "depth_2"
N = 4
F32 = jnp.float32
BF16 = jnp.bfloat16
LIMIT = 24 * 2**20
VMEM = pl.BlockSpec(memory_space=pltpu.VMEM)


def run(body, args, outs, scratch=(), flops=0):
    nbytes = sum(a.size * a.dtype.itemsize for a in args)
    return pl.pallas_call(
        body,
        out_shape=[jax.ShapeDtypeStruct(s, t) for s, t in outs],
        in_specs=[VMEM] * len(args),
        out_specs=[VMEM] * len(outs),
        scratch_shapes=[pltpu.VMEM(s, t) for s, t in scratch],
        cost_estimate=pl.CostEstimate(flops=flops, bytes_accessed=nbytes, transcendentals=0),
        compiler_params=pltpu.CompilerParams(vmem_limit_bytes=LIMIT),
    )(*args)


def section():
    return lax.axis_index("section")


def core():
    return lax.axis_index(CORE)


def split(x):
    high = x.astype(BF16)
    return high, (x - high.astype(F32)).astype(BF16)


def columns():
    return lax.broadcasted_iota(jnp.int32, (C, H * W), 1)


def across(x):
    place = columns()
    left = jnp.where(place % W == 0, 0.0, pltpu.roll(x, 1, 1))
    right = jnp.where(place % W == W - 1, 0.0, pltpu.roll(x, H * W - 1, 1))
    return jnp.concatenate([left, x, right], axis=0)


def down(x):
    return jnp.where(columns() < W, 0.0, pltpu.roll(x, W, 1))


def up(x):
    return jnp.where(columns() >= H * W - W, 0.0, pltpu.roll(x, H * W - W, 1))


def dot(a, b):
    return jnp.dot(a, b, preferred_element_type=F32)


def conv(taps, high, low):
    first = dot(taps, high)
    z = first[:192] + first[192:] + dot(taps[:192], low)
    return z[C : 2 * C] + down(z[:C]) + up(z[2 * C :])


def silu_slope(preact):
    gate = 1.0 / (1.0 + jnp.exp(-preact))
    return gate * (1.0 + preact * (1.0 - gate))


def prepare_body(f_ref, forward_ref, mine_ref, yours_ref, back):
    for b in range(3):
        rows = slice(b * C, b * C + C)
        low_rows = slice(192 + b * C, 192 + b * C + C)
        taps = [f_ref[0, a * 9 + b * 3 + cc] for a in range(3) for cc in range(3)]
        high, low = split(jnp.concatenate(taps, axis=1))
        forward_ref[rows] = high
        forward_ref[low_rows] = low
        taps = [f_ref[0, (2 - a) * 9 + (2 - b) * 3 + 2 - cc] for a in range(3) for cc in range(3)]
        back[rows] = jnp.concatenate(taps, axis=0).T
    c = core()
    mine_ref[...] = back[pl.ds(pl.multiple_of(c * 96, 32), 96)]
    yours_ref[...] = back[pl.ds(pl.multiple_of((1 - c) * 96, 32), 96)]


def slope_body(ks, act_ref, inner_ref, outer_ref, taps_ref, *refs):
    c = core()
    for i, k in enumerate(ks):
        m = section() ^ k
        out, vh_ref, vl_ref = refs[3 * i : 3 * i + 3]
        for e in range(4):
            if e == 0:
                x = jnp.where(c == 0, outer_ref[m], inner_ref[m])
            elif e == 3:
                x = jnp.where(c == 0, inner_ref[m], outer_ref[m])
            else:
                x = act_ref[m, e - 1]
            high, low = split(across(x))
            vh_ref[e] = high
            vl_ref[e] = low
        for d in range(2):
            z = conv(taps_ref[...], vh_ref[d : d + 3].reshape(576, 256), vl_ref[d : d + 3].reshape(576, 256))
            out[d] = silu_slope(z)


def chosen(index, refs, *at):
    out = refs[0][at]
    for k in range(1, len(refs)):
        out = jnp.where(index == k, refs[k][at], out)
    return out


def by_core(even, odd):
    return jnp.where(core() == 0, even, odd)


def pick_body(d0, d1, d2, d3, cot_ref, s3_ref, inner_ref, outer_ref, one_ref, two_ref):
    m = section()
    refs = (d0, d1, d2, d3)
    top = [cot_ref[m, d] * chosen(m ^ 3, refs, d) for d in range(2)]
    face = [chosen(m ^ 1, refs, d) for d in range(2)]
    for d in range(2):
        s3_ref[d] = top[d]
        below = chosen(m ^ 2, refs, d)
        for ref in (inner_ref, outer_ref):
            ref[d] = top[d]
            ref[2 + d] = below
    inner_ref[4] = by_core(face[1], face[0])
    outer_ref[4] = by_core(face[0], face[1])
    even = lax.rem(lax.axis_index("depth_1"), 2) == 0
    one_ref[0] = jnp.where(even, top[1], top[0])
    two_ref[0] = jnp.where(even, top[0], top[1])


def above_body(one_ref, three_ref, out_ref):
    out_ref[...] = jnp.where(lax.rem(section(), 2) == 0, one_ref[...], three_ref[...])


def taps_body(mine_ref, yours_ref, one_ref, three_ref, far_ref, other_ref, out_ref):
    s = section()
    c = core()

    def put(layer, row, x):
        high, low = split(x)
        size = x.shape[0]
        out_ref[layer, pl.ds(row, size)] = high
        out_ref[layer, pl.ds(192 + row, size)] = low

    mine = pl.multiple_of(c * 96, 32)
    yours = pl.multiple_of((1 - c) * 96, 32)
    put(s, mine, mine_ref[...])
    put(s, yours, yours_ref[...])
    put(s ^ 1, mine, one_ref[...])
    put(s ^ 3, mine, three_ref[...])
    put(s ^ 2, mine, far_ref[...])
    put(s ^ 1, yours, other_ref[0:96])
    put(s ^ 3, yours, other_ref[96:192])
    put(s ^ 2, yours, other_ref[192:288])


def store(x, high_ref, low_ref, at):
    high, low = split(across(x))
    high_ref[at] = high
    low_ref[at] = low


def convs(taps_ref, layer, high_ref, low_ref, count):
    return [
        conv(taps_ref[layer], high_ref[d : d + 3].reshape(576, 256), low_ref[d : d + 3].reshape(576, 256))
        for d in range(count)
    ]


def chain_body(inner_in, outer_in, one_in, two_in, d0, d1, d2, d3, s3, taps_ref, *refs):
    o, ig3, ig2, ig1, s0, inner_ref, outer_ref, s2, s1, ah, al, bh, bl, ch, cl = refs[:4], *refs[4:]
    m = section()
    factors = (d0, d1, d2, d3)
    even = lax.rem(lax.axis_index("depth_1"), 2) == 0

    def left(e):
        return by_core(outer_in[e], inner_in[e])

    def right(e):
        return by_core(inner_in[e], outer_in[e])

    planes = [jnp.where(even, two_in[0], one_in[0]), left(0), left(1), s3[0], s3[1]]
    planes += [right(0), right(1), jnp.where(even, one_in[0], two_in[0])]
    for e, x in enumerate(planes):
        store(x, ah, al, e)
    for e, g in enumerate(convs(taps_ref, 3, ah, al, 6)):
        if e < 2:
            slope = g * left(2 + e)
        elif e > 3:
            slope = g * right(e - 2)
        else:
            slope = g * chosen(m ^ 2, factors, e - 2)
            ig3[e - 2] = g
            s2[e - 2] = slope
        store(slope, bh, bl, e)
    for e, g in enumerate(convs(taps_ref, 2, bh, bl, 4)):
        if e == 0:
            slope = g * left(4)
        elif e == 3:
            slope = g * right(4)
        else:
            slope = g * chosen(m ^ 1, factors, e - 1)
            ig2[e - 1] = g
            s1[e - 1] = slope
        store(slope, ch, cl, e)
    for d, g in enumerate(convs(taps_ref, 1, ch, cl, 2)):
        ig1[d] = g
        s0[d] = g * chosen(m, factors, d)
    for d in range(2):
        for k in range(N):
            o[k][d] = chosen(m ^ k, (s0, s1, s2, s3), d)
    inner_ref[0] = by_core(s0[1], s0[0])
    outer_ref[0] = by_core(s0[0], s0[1])


def last_body(inner_in, outer_in, s0, ig3, ig2, ig1, taps_ref, p0, p1, p2, p3, ig0, vh, vl):
    m = section()
    for e, x in enumerate((by_core(outer_in[0], inner_in[0]), s0[0], s0[1], by_core(inner_in[0], outer_in[0]))):
        store(x, vh, vl, e)
    for d, g in enumerate(convs(taps_ref, 0, vh, vl, 2)):
        ig0[d] = g
    for d in range(2):
        for k, p in enumerate((p0, p1, p2, p3)):
            p[d] = chosen(m ^ k, (ig0, ig1, ig2, ig3), d)


def filter_body(*refs):
    keep_ref, send_ref, acc = refs[12:]
    c = core()
    nt = (((1,), (1,)), ((), ()))
    both, high_only, right_high, right_low = [], [], [], []
    for k in range(N):
        ref, vh_ref, vl_ref = refs[3 * k : 3 * k + 3]
        for d in range(2):
            x = ref[d]
            high, low = split(jnp.concatenate([up(x), x, down(x)], axis=0))
            both.append(jnp.concatenate([high, low], axis=0))
            high_only.append(high)
            right_high.append(vh_ref[d : d + 3].reshape(576, 256))
            right_low.append(vl_ref[d : d + 3].reshape(576, 256))
    first = lax.dot_general(
        jnp.concatenate(both, axis=1), jnp.concatenate(right_high, axis=1), nt, preferred_element_type=F32
    )
    second = lax.dot_general(
        jnp.concatenate(high_only, axis=1), jnp.concatenate(right_low, axis=1), nt, preferred_element_type=F32
    )
    acc[...] = first[:192] + first[192:] + second

    def piece(row, size):
        if row < 768:
            j = row // 192
            return acc[row - j * 192 : row - j * 192 + size, j * 128 : (j + 1) * 128]
        r = row - 768
        return jnp.concatenate([acc[r : r + size, 512:576], acc[r + 96 : r + 96 + size, 512:576]], axis=1)

    for half in range(2):

        def fill(ref):
            row = 432 * half
            stop = row + 432
            while row < stop:
                size = min((row // 192 + 1) * 192 if row < 768 else 864, stop) - row
                ref[row - 432 * half : row - 432 * half + size] = piece(row, size)
                row += size
            ref[432:512] = jnp.zeros((80, 128), F32)

        @pl.when(c == half)
        def _():
            fill(keep_ref)

        @pl.when(c != half)
        def _():
            fill(send_ref)


def finish_body(own_ref, other_ref, out_ref, full):
    c = core()
    full[pl.ds(pl.multiple_of(c * 432, 8), 432)] = own_ref[0:432]
    full[pl.ds(pl.multiple_of((1 - c) * 432, 8), 432)] = other_ref[0:432]
    for a in range(3):
        for b in range(3):
            for cc in range(3):
                block = a * 3 + cc
                if block < 8:
                    x = full[(block // 2) * 192 + b * C : (block // 2) * 192 + b * C + C]
                    x = x[:, (block % 2) * C : (block % 2) * C + C]
                    out_ref[0, a * 9 + b * 3 + cc] = x
                else:
                    for part in range(2):
                        row = b * C + part * 32
                        side = 0 if row < 96 else 1
                        x = full[768 + row - 96 * side : 768 + row - 96 * side + 32, side * C : side * C + C]
                        out_ref[0, a * 9 + b * 3 + cc, part * 32 : part * 32 + 32] = x


def gather_body(x0, x1, x2, x3, out_ref):
    s = section()
    for k, ref in enumerate((x0, x1, x2, x3)):
        out_ref[0, s ^ k] = ref[...]


def met(x, k):
    return lax.ppermute(x, "section", [(i, i ^ k) for i in range(N)])


def handed(parts):
    return [parts[0]] + [met(parts[k], k) for k in (1, 2, 3)]


def swapped(x):
    return lax.ppermute(x, CORE, [(0, 1), (1, 0)])


def neighbours(inner, outer):
    count = lax.axis_size(DEPTH)
    inner = swapped(inner)
    pairs = [(i, i + 1) for i in range(1, count - 1, 2)]
    outer = lax.ppermute(outer, DEPTH, pairs + [(j, i) for i, j in pairs])
    return inner, outer


def skipped(one, two):
    count = lax.axis_size(DEPTH)
    out = []
    for x, first in ((one, 0), (two, 2)):
        pairs = [(i + c, i + c + 2) for i in range(first, count - 2, 4) for c in range(2)]
        out.append(lax.ppermute(x, DEPTH, pairs + [(j, i) for i, j in pairs]))
    return out


def window(activations, filters, cotangent):
    c = lax.axis_index(CORE)
    act = activations[0]
    plane = (C, H * W)
    two = ((2, *plane), F32)

    inner = lax.dynamic_index_in_dim(act, 1 - c, 1, keepdims=False)
    outer = lax.dynamic_index_in_dim(act, c, 1, keepdims=False)
    inner, outer = neighbours(inner, outer)
    forward, mine, yours = run(
        prepare_body,
        (filters,),
        [((384, 576), BF16), ((96, 576), F32), ((96, 576), F32)],
        [((192, 576), F32)],
        flops=10**6,
    )
    factors, shifted = [None] * N, [None] * N
    for ks in ((2,), (1, 3), (0,)):
        out = run(
            functools.partial(slope_body, ks),
            (act, inner, outer, forward),
            [two, ((4, 192, 256), BF16), ((4, 192, 256), BF16)] * len(ks),
            flops=2 * 2 * 192 * 576 * 256 * 3 * len(ks),
        )
        for i, k in enumerate(ks):
            factors[k], *shifted[k] = out[3 * i : 3 * i + 3]
    factors = handed(factors)

    one = met(mine, 1)
    three_half = met(mine, 3)
    (above,) = run(above_body, (one, three_half), [((96, 576), F32)], flops=10**6)
    far = lax.ppermute(above, "section", [(i, (i - 1) % N) for i in range(N)])
    other = swapped(jnp.concatenate([one, three_half, far], axis=0))
    (taps,) = run(taps_body, (mine, yours, one, three_half, far, other), [((N, 384, 576), BF16)], flops=10**6)

    one_plane = ((1, *plane), F32)
    five = ((5, *plane), F32)
    s3, inner, outer, one, two_apart = run(
        pick_body, (*factors, cotangent), [two, five, five, one_plane, one_plane], flops=10**6
    )
    inner, outer = neighbours(inner, outer)
    one, two_apart = skipped(one, two_apart)
    shifted_planes = [((e, 192, 256), BF16) for e in (8, 8, 6, 6, 4, 4)]
    *packed, ig3, ig2, ig1, s0, inner, outer = run(
        chain_body,
        (inner, outer, one, two_apart, *factors, s3, taps),
        [two] * 8 + [one_plane] * 2,
        [((2, *plane), F32)] * 2 + shifted_planes,
        flops=2 * 12 * 192 * 576 * 256 * 3,
    )
    slopes = handed(packed)
    inner, outer = neighbours(inner, outer)
    packed = run(
        last_body,
        (inner, outer, s0, ig3, ig2, ig1, taps),
        [two] * 4,
        [((2, *plane), F32)] + shifted_planes[4:],
        flops=2 * 2 * 192 * 576 * 256 * 3,
    )
    grads = handed(packed)

    keep, send = run(
        filter_body,
        tuple(x for k in range(N) for x in (slopes[k], *shifted[k])),
        [((512, 128), F32)] * 2,
        [((192, 576), F32)],
        flops=2 * 8 * 192 * 576 * 256 * 3,
    )
    part = (keep + swapped(send)).reshape(32, 16, 128)
    part = lax.all_to_all(part, PLANE, 0, 0, tiled=True)
    scaling = 1.0 / math.sqrt(N * 2 * lax.axis_size(DEPTH) * H * W)
    total = jnp.sum(part, axis=0) * scaling
    part = lax.all_to_all(jnp.broadcast_to(total[None], (32, 16, 128)), PLANE, 0, 0, tiled=True)
    part = part.reshape(512, 128)
    other_part = swapped(part)
    (filter_grads,) = run(finish_body, (part, other_part), [((1, 27, C, C), F32)], [((864, 128), F32)], flops=10**6)
    (input_grads,) = run(gather_body, (*grads,), [((1, N, 2, *plane), F32)], flops=10**6)
    return input_grads, filter_grads


def solution(mesh):
    finer = Mesh(
        mesh.devices.reshape(mesh.shape["section"], 8, 4, 2),
        ("section", "depth_0", "depth_1", "depth_2"),
    )
    placed = (
        P("section", None, DEPTH, None, None),
        P("section", None, None, None),
        P(None, DEPTH, None, None),
    )
    return jax.shard_map(
        window,
        mesh=finer,
        in_specs=placed,
        out_specs=(P("section", None, DEPTH, None, None), P("section", None, None, None)),
        check_vma=False,
    )
```

```python
import functools
import math

import jax
import jax.numpy as jnp
from jax import lax
from jax.experimental import pallas as pl
from jax.experimental.pallas import tpu as pltpu
from jax.sharding import Mesh
from jax.sharding import PartitionSpec as P


H = 16
W = 16
C = 64
DEPTH = ("depth_0", "depth_1", "depth_2")
PLANE = ("depth_0", "depth_1")
CORE = "depth_2"
N = 4
F32 = jnp.float32
BF16 = jnp.bfloat16
LIMIT = 24 * 2**20
VMEM = pl.BlockSpec(memory_space=pltpu.VMEM)


def run(body, args, outs, scratch=(), flops=0):
    nbytes = sum(a.size * a.dtype.itemsize for a in args)
    return pl.pallas_call(
        body,
        out_shape=[jax.ShapeDtypeStruct(s, t) for s, t in outs],
        in_specs=[VMEM] * len(args),
        out_specs=[VMEM] * len(outs),
        scratch_shapes=[pltpu.VMEM(s, t) for s, t in scratch],
        cost_estimate=pl.CostEstimate(flops=flops, bytes_accessed=nbytes, transcendentals=0),
        compiler_params=pltpu.CompilerParams(vmem_limit_bytes=LIMIT),
    )(*args)


def section():
    return lax.axis_index("section")


def core():
    return lax.axis_index(CORE)


def split(x):
    high = x.astype(BF16)
    return high, (x - high.astype(F32)).astype(BF16)


def columns():
    return lax.broadcasted_iota(jnp.int32, (C, H * W), 1)


def across(x):
    place = columns()
    left = jnp.where(place % W == 0, 0.0, pltpu.roll(x, 1, 1))
    right = jnp.where(place % W == W - 1, 0.0, pltpu.roll(x, H * W - 1, 1))
    return jnp.concatenate([left, x, right], axis=0)


def down(x):
    return jnp.where(columns() < W, 0.0, pltpu.roll(x, W, 1))


def up(x):
    return jnp.where(columns() >= H * W - W, 0.0, pltpu.roll(x, H * W - W, 1))


def dot(a, b):
    return jnp.dot(a, b, preferred_element_type=F32)


def conv(taps, high, low):
    first = dot(taps, high)
    z = first[:192] + first[192:] + dot(taps[:192], low)
    return z[C : 2 * C] + down(z[:C]) + up(z[2 * C :])


def conv_wide(taps, high, low):
    z = dot(taps, jnp.concatenate([high, high, low], axis=0))
    return z[C : 2 * C] + down(z[:C]) + up(z[2 * C :])


def silu_slope(preact):
    gate = 1.0 / (1.0 + jnp.exp(-preact))
    return gate * (1.0 + preact * (1.0 - gate))


def prepare_body(f_ref, forward_ref, mine_ref, yours_ref, back):
    for b in range(3):
        rows = slice(b * C, b * C + C)
        taps = [f_ref[0, a * 9 + b * 3 + cc] for a in range(3) for cc in range(3)]
        high, low = split(jnp.concatenate(taps, axis=1))
        forward_ref[rows] = jnp.concatenate([high, low, high], axis=1)
        taps = [f_ref[0, (2 - a) * 9 + (2 - b) * 3 + 2 - cc] for a in range(3) for cc in range(3)]
        back[rows] = jnp.concatenate(taps, axis=0).T
    c = core()
    mine_ref[...] = back[pl.ds(pl.multiple_of(c * 96, 32), 96)]
    yours_ref[...] = back[pl.ds(pl.multiple_of((1 - c) * 96, 32), 96)]


def slope_body(ks, act_ref, inner_ref, outer_ref, taps_ref, *refs):
    c = core()
    for i, k in enumerate(ks):
        m = section() ^ k
        out, vh_ref, vl_ref = refs[3 * i : 3 * i + 3]
        for e in range(4):
            if e == 0:
                x = jnp.where(c == 0, outer_ref[m], inner_ref[m])
            elif e == 3:
                x = jnp.where(c == 0, inner_ref[m], outer_ref[m])
            else:
                x = act_ref[m, e - 1]
            high, low = split(across(x))
            vh_ref[e] = high
            vl_ref[e] = low
        for d in range(2):
            z = conv_wide(taps_ref[...], vh_ref[d : d + 3].reshape(576, 256), vl_ref[d : d + 3].reshape(576, 256))
            out[d] = silu_slope(z)


def chosen(index, refs, *at):
    out = refs[0][at]
    for k in range(1, len(refs)):
        out = jnp.where(index == k, refs[k][at], out)
    return out


def by_core(even, odd):
    return jnp.where(core() == 0, even, odd)


def pick_body(d0, d1, d2, d3, cot_ref, s3_ref, inner_ref, outer_ref, one_ref, two_ref):
    m = section()
    refs = (d0, d1, d2, d3)
    top = [cot_ref[m, d] * chosen(m ^ 3, refs, d) for d in range(2)]
    face = [chosen(m ^ 1, refs, d) for d in range(2)]
    for d in range(2):
        s3_ref[d] = top[d]
        below = chosen(m ^ 2, refs, d)
        for ref in (inner_ref, outer_ref):
            ref[d] = top[d]
            ref[2 + d] = below
    inner_ref[4] = by_core(face[1], face[0])
    outer_ref[4] = by_core(face[0], face[1])
    even = lax.rem(lax.axis_index("depth_1"), 2) == 0
    one_ref[0] = jnp.where(even, top[1], top[0])
    two_ref[0] = jnp.where(even, top[0], top[1])


def above_body(one_ref, three_ref, out_ref):
    out_ref[...] = jnp.where(lax.rem(section(), 2) == 0, one_ref[...], three_ref[...])


def taps_body(mine_ref, yours_ref, one_ref, three_ref, far_ref, other_ref, out_ref):
    s = section()
    c = core()

    def put(layer, row, x):
        high, low = split(x)
        size = x.shape[0]
        out_ref[layer, pl.ds(row, size)] = high
        out_ref[layer, pl.ds(192 + row, size)] = low

    mine = pl.multiple_of(c * 96, 32)
    yours = pl.multiple_of((1 - c) * 96, 32)
    put(s, mine, mine_ref[...])
    put(s, yours, yours_ref[...])
    put(s ^ 1, mine, one_ref[...])
    put(s ^ 3, mine, three_ref[...])
    put(s ^ 2, mine, far_ref[...])
    put(s ^ 1, yours, other_ref[0:96])
    put(s ^ 3, yours, other_ref[96:192])
    put(s ^ 2, yours, other_ref[192:288])


def store(x, high_ref, low_ref, at):
    high, low = split(across(x))
    high_ref[at] = high
    low_ref[at] = low


def convs(taps_ref, layer, high_ref, low_ref, count):
    return [
        conv(taps_ref[layer], high_ref[d : d + 3].reshape(576, 256), low_ref[d : d + 3].reshape(576, 256))
        for d in range(count)
    ]


def chain_body(inner_in, outer_in, one_in, two_in, d0, d1, d2, d3, s3, taps_ref, *refs):
    o, ig3, ig2, ig1, s0, inner_ref, outer_ref, s2, s1, ah, al, bh, bl, ch, cl = refs[:4], *refs[4:]
    m = section()
    factors = (d0, d1, d2, d3)
    even = lax.rem(lax.axis_index("depth_1"), 2) == 0

    def left(e):
        return by_core(outer_in[e], inner_in[e])

    def right(e):
        return by_core(inner_in[e], outer_in[e])

    planes = [jnp.where(even, two_in[0], one_in[0]), left(0), left(1), s3[0], s3[1]]
    planes += [right(0), right(1), jnp.where(even, one_in[0], two_in[0])]
    for e, x in enumerate(planes):
        store(x, ah, al, e)
    for e, g in enumerate(convs(taps_ref, 3, ah, al, 6)):
        if e < 2:
            slope = g * left(2 + e)
        elif e > 3:
            slope = g * right(e - 2)
        else:
            slope = g * chosen(m ^ 2, factors, e - 2)
            ig3[e - 2] = g
            s2[e - 2] = slope
        store(slope, bh, bl, e)
    for e, g in enumerate(convs(taps_ref, 2, bh, bl, 4)):
        if e == 0:
            slope = g * left(4)
        elif e == 3:
            slope = g * right(4)
        else:
            slope = g * chosen(m ^ 1, factors, e - 1)
            ig2[e - 1] = g
            s1[e - 1] = slope
        store(slope, ch, cl, e)
    for d, g in enumerate(convs(taps_ref, 1, ch, cl, 2)):
        ig1[d] = g
        s0[d] = g * chosen(m, factors, d)
    for d in range(2):
        for k in range(N):
            o[k][d] = chosen(m ^ k, (s0, s1, s2, s3), d)
    inner_ref[0] = by_core(s0[1], s0[0])
    outer_ref[0] = by_core(s0[0], s0[1])


def last_body(inner_in, outer_in, s0, ig3, ig2, ig1, taps_ref, p0, p1, p2, p3, ig0, vh, vl):
    m = section()
    for e, x in enumerate((by_core(outer_in[0], inner_in[0]), s0[0], s0[1], by_core(inner_in[0], outer_in[0]))):
        store(x, vh, vl, e)
    for d, g in enumerate(convs(taps_ref, 0, vh, vl, 2)):
        ig0[d] = g
    for d in range(2):
        for k, p in enumerate((p0, p1, p2, p3)):
            p[d] = chosen(m ^ k, (ig0, ig1, ig2, ig3), d)


def filter_body(*refs):
    keep_ref, send_ref, acc = refs[12:]
    c = core()
    nt = (((1,), (1,)), ((), ()))
    both, high_only, right_high, right_low = [], [], [], []
    for k in range(N):
        ref, vh_ref, vl_ref = refs[3 * k : 3 * k + 3]
        for d in range(2):
            x = ref[d]
            high, low = split(jnp.concatenate([up(x), x, down(x)], axis=0))
            both.append(jnp.concatenate([high, low], axis=0))
            high_only.append(high)
            right_high.append(vh_ref[d : d + 3].reshape(576, 256))
            right_low.append(vl_ref[d : d + 3].reshape(576, 256))
    first = lax.dot_general(
        jnp.concatenate(both, axis=1), jnp.concatenate(right_high, axis=1), nt, preferred_element_type=F32
    )
    second = lax.dot_general(
        jnp.concatenate(high_only, axis=1), jnp.concatenate(right_low, axis=1), nt, preferred_element_type=F32
    )
    acc[...] = first[:192] + first[192:] + second

    def piece(row, size):
        if row < 768:
            j = row // 192
            return acc[row - j * 192 : row - j * 192 + size, j * 128 : (j + 1) * 128]
        r = row - 768
        return jnp.concatenate([acc[r : r + size, 512:576], acc[r + 96 : r + 96 + size, 512:576]], axis=1)

    for half in range(2):

        def fill(ref):
            row = 432 * half
            stop = row + 432
            while row < stop:
                size = min((row // 192 + 1) * 192 if row < 768 else 864, stop) - row
                ref[row - 432 * half : row - 432 * half + size] = piece(row, size)
                row += size
            ref[432:512] = jnp.zeros((80, 128), F32)

        @pl.when(c == half)
        def _():
            fill(keep_ref)

        @pl.when(c != half)
        def _():
            fill(send_ref)


def finish_body(own_ref, other_ref, out_ref, full):
    c = core()
    full[pl.ds(pl.multiple_of(c * 432, 8), 432)] = own_ref[0:432]
    full[pl.ds(pl.multiple_of((1 - c) * 432, 8), 432)] = other_ref[0:432]
    for a in range(3):
        for b in range(3):
            for cc in range(3):
                block = a * 3 + cc
                if block < 8:
                    x = full[(block // 2) * 192 + b * C : (block // 2) * 192 + b * C + C]
                    x = x[:, (block % 2) * C : (block % 2) * C + C]
                    out_ref[0, a * 9 + b * 3 + cc] = x
                else:
                    for part in range(2):
                        row = b * C + part * 32
                        side = 0 if row < 96 else 1
                        x = full[768 + row - 96 * side : 768 + row - 96 * side + 32, side * C : side * C + C]
                        out_ref[0, a * 9 + b * 3 + cc, part * 32 : part * 32 + 32] = x


def gather_body(x0, x1, x2, x3, out_ref):
    s = section()
    for k, ref in enumerate((x0, x1, x2, x3)):
        out_ref[0, s ^ k] = ref[...]


def met(x, k):
    return lax.ppermute(x, "section", [(i, i ^ k) for i in range(N)])


def handed(parts):
    return [parts[0]] + [met(parts[k], k) for k in (1, 2, 3)]


def swapped(x):
    return lax.ppermute(x, CORE, [(0, 1), (1, 0)])


def neighbours(inner, outer):
    count = lax.axis_size(DEPTH)
    inner = swapped(inner)
    pairs = [(i, i + 1) for i in range(1, count - 1, 2)]
    outer = lax.ppermute(outer, DEPTH, pairs + [(j, i) for i, j in pairs])
    return inner, outer


def skipped(one, two):
    count = lax.axis_size(DEPTH)
    out = []
    for x, first in ((one, 0), (two, 2)):
        pairs = [(i + c, i + c + 2) for i in range(first, count - 2, 4) for c in range(2)]
        out.append(lax.ppermute(x, DEPTH, pairs + [(j, i) for i, j in pairs]))
    return out


def window(activations, filters, cotangent):
    c = lax.axis_index(CORE)
    act = activations[0]
    plane = (C, H * W)
    two = ((2, *plane), F32)

    inner = lax.dynamic_index_in_dim(act, 1 - c, 1, keepdims=False)
    outer = lax.dynamic_index_in_dim(act, c, 1, keepdims=False)
    inner, outer = neighbours(inner, outer)
    forward, mine, yours = run(
        prepare_body,
        (filters,),
        [((192, 1728), BF16), ((96, 576), F32), ((96, 576), F32)],
        [((192, 576), F32)],
        flops=10**6,
    )
    factors, shifted = [None] * N, [None] * N
    for ks in ((2,), (1, 3), (0,)):
        out = run(
            functools.partial(slope_body, ks),
            (act, inner, outer, forward),
            [two, ((4, 192, 256), BF16), ((4, 192, 256), BF16)] * len(ks),
            flops=2 * 2 * 192 * 576 * 256 * 3 * len(ks),
        )
        for i, k in enumerate(ks):
            factors[k], *shifted[k] = out[3 * i : 3 * i + 3]
    factors = handed(factors)

    one = met(mine, 1)
    three_half = met(mine, 3)
    (above,) = run(above_body, (one, three_half), [((96, 576), F32)], flops=10**6)
    far = lax.ppermute(above, "section", [(i, (i - 1) % N) for i in range(N)])
    other = swapped(jnp.concatenate([one, three_half, far], axis=0))
    (taps,) = run(taps_body, (mine, yours, one, three_half, far, other), [((N, 384, 576), BF16)], flops=10**6)

    one_plane = ((1, *plane), F32)
    five = ((5, *plane), F32)
    s3, inner, outer, one, two_apart = run(
        pick_body, (*factors, cotangent), [two, five, five, one_plane, one_plane], flops=10**6
    )
    inner, outer = neighbours(inner, outer)
    one, two_apart = skipped(one, two_apart)
    shifted_planes = [((e, 192, 256), BF16) for e in (8, 8, 6, 6, 4, 4)]
    *packed, ig3, ig2, ig1, s0, inner, outer = run(
        chain_body,
        (inner, outer, one, two_apart, *factors, s3, taps),
        [two] * 8 + [one_plane] * 2,
        [((2, *plane), F32)] * 2 + shifted_planes,
        flops=2 * 12 * 192 * 576 * 256 * 3,
    )
    slopes = handed(packed)
    inner, outer = neighbours(inner, outer)
    packed = run(
        last_body,
        (inner, outer, s0, ig3, ig2, ig1, taps),
        [two] * 4,
        [((2, *plane), F32)] + shifted_planes[4:],
        flops=2 * 2 * 192 * 576 * 256 * 3,
    )
    grads = handed(packed)

    keep, send = run(
        filter_body,
        tuple(x for k in range(N) for x in (slopes[k], *shifted[k])),
        [((512, 128), F32)] * 2,
        [((192, 576), F32)],
        flops=2 * 8 * 192 * 576 * 256 * 3,
    )
    part = (keep + swapped(send)).reshape(32, 16, 128)
    part = lax.all_to_all(part, PLANE, 0, 0, tiled=True)
    scaling = 1.0 / math.sqrt(N * 2 * lax.axis_size(DEPTH) * H * W)
    total = jnp.sum(part, axis=0) * scaling
    part = lax.all_to_all(jnp.broadcast_to(total[None], (32, 16, 128)), PLANE, 0, 0, tiled=True)
    part = part.reshape(512, 128)
    other_part = swapped(part)
    (filter_grads,) = run(finish_body, (part, other_part), [((1, 27, C, C), F32)], [((864, 128), F32)], flops=10**6)
    (input_grads,) = run(gather_body, (*grads,), [((1, N, 2, *plane), F32)], flops=10**6)
    return input_grads, filter_grads


def solution(mesh):
    finer = Mesh(
        mesh.devices.reshape(mesh.shape["section"], 8, 4, 2),
        ("section", "depth_0", "depth_1", "depth_2"),
    )
    placed = (
        P("section", None, DEPTH, None, None),
        P("section", None, None, None),
        P(None, DEPTH, None, None),
    )
    return jax.shard_map(
        window,
        mesh=finer,
        in_specs=placed,
        out_specs=(P("section", None, DEPTH, None, None), P("section", None, None, None)),
        check_vma=False,
    )
```
